512 devices in a mesh: ctx: 64 (over x, z_hi, y), ch: 8 (over z_lo, core).
Axes of the slice: x: 4, y: 4, z: 16 (z_hi: 4, z_lo: 4; z = z_hi * 4 + z_lo), core: 2. Of those that a mesh axis runs over, the one named last changes fastest.
Arguments:
- value_in: bfloat16 [8192, 4096], P('ctx', 'ch'), may hold values from -6 to 6
- key_in: bfloat16 [8192, 4096], P('ctx', 'ch'), may hold values from -6 to 6
- gate_short: bfloat16 [8192, 4096], P('ctx', 'ch'), may hold values from -6 to 6
- gate_long: bfloat16 [8192, 4096], P('ctx', 'ch'), may hold values from -6 to 6
- short_filter: bfloat16 [256, 128], P('ch'), may hold values from -0.5 to 0.5
- long_filter: float32 [4096, 8192], P(('ch', 'ctx')), may hold values from -2 to 2
- skip_gain: float32 [4096], P('ch'), may hold values from 0.5 to 1.5
- out_weight: bfloat16 [4096, 4096], P('ctx', 'ch'), may hold values from -0.09375 to 0.09375
Outputs:
- layer_out: bfloat16 [8192, 4096], P('ctx', 'ch')
The draws below stay inside these ranges and needn't reach their ends.
All inputs are finite; a program needn't handle non-finite values.
Results may differ from the reference program's by a relative error of at most 0.0067.
Values may be sent and summed in bfloat16 or wider, within the bound.
No kernel may reach another device: no remote copies, remote signals or barrier semaphores. Data moves between devices by JAX's collectives and lax.ppermute only.
A program may use at most 64 MiB of HBM per device.

```python
import jax
import jax.numpy as jnp
from jax import lax

MODEL_WIDTH = 4096
GSIZE = 16
TAPS = 128
SEQUENCE_TOKENS = 8192
GROUPS = 256


def draw_long_filter(key, part):
    random_subkeys = jax.random.split(jax.random.fold_in(key, 17), 8)
    delay_offsets = jnp.arange(SEQUENCE_TOKENS, dtype=jnp.float32)
    fast_share = 0.3
    quick_mask = jax.random.uniform(random_subkeys[0], (MODEL_WIDTH,)) < fast_share
    quick_rate = jnp.exp(jax.random.uniform(random_subkeys[1], (MODEL_WIDTH,), minval=jnp.log(1.0 / 50.0), maxval=jnp.log(1.0 / 30.0)))
    steady_rate = jnp.exp(jax.random.uniform(random_subkeys[2], (MODEL_WIDTH,), minval=jnp.log(0.1 / SEQUENCE_TOKENS), maxval=jnp.log(1.0 / SEQUENCE_TOKENS)))
    decay_rate = jnp.where(quick_mask, quick_rate, steady_rate)
    decay_profile = jnp.exp(-decay_rate[:, None] * delay_offsets[None, :])
    for spike_pulse in range(2):
        spike_position = jax.random.randint(random_subkeys[3 + spike_pulse], (MODEL_WIDTH, 1), 1, SEQUENCE_TOKENS).astype(jnp.float32)
        spike_retained = jax.random.uniform(random_subkeys[5 + spike_pulse], (MODEL_WIDTH, 1), minval=0.6, maxval=0.85)
        decay_profile = decay_profile * jnp.where(delay_offsets[None, :] >= spike_position, spike_retained, 1.0)
    jitter = jnp.clip(jax.random.normal(random_subkeys[7], (MODEL_WIDTH, SEQUENCE_TOKENS)), -4.0, 4.0)
    norm_scale = 1.0 / jnp.sqrt(jnp.sum(decay_profile * decay_profile, axis=1, keepdims=True))
    return (jitter * decay_profile * norm_scale).astype(jnp.float32)


def level_of(own_key, shape, shards, least, top_value):
    level, own = 1.0, jax.random.fold_in(own_key, 6)
    for axis_at, parts in shards:
        draws = jnp.exp(jax.random.uniform(jax.random.fold_in(own, axis_at), (parts,), jnp.float32, least / len(shards), top_value / len(shards)))
        level = level * jnp.repeat(draws, shape[axis_at] // parts).reshape([-1 if axis == axis_at else 1 for axis in range(len(shape))])
    return level


def centred(own_key, shape, scale, limit, pieces=(), held_as=jnp.bfloat16):
    array = scale * jax.random.normal(own_key, shape, jnp.float32)
    if pieces:
        array = array * level_of(own_key, shape, pieces, -0.22, 0.18)
    return jnp.clip(array, -limit, limit).astype(held_as)


def setup_inputs(seed: int = 0) -> dict:
    splits = jax.random.split(jax.random.key(seed), 9)
    value_in = centred(splits[0], (SEQUENCE_TOKENS, MODEL_WIDTH), 1.0, 6.0, ((0, 64), (1, 8)))
    key_in = centred(splits[1], (SEQUENCE_TOKENS, MODEL_WIDTH), 1.0, 6.0, ((0, 64), (1, 8)))
    gate_short = centred(splits[2], (SEQUENCE_TOKENS, MODEL_WIDTH), 1.0, 6.0, ((0, 64), (1, 8)))
    gate_long = centred(splits[3], (SEQUENCE_TOKENS, MODEL_WIDTH), 1.0, 6.0, ((0, 64), (1, 8)))
    short_filter = centred(splits[4], (GROUPS, TAPS), TAPS ** -0.5, 0.5, ((0, 8),))
    long_filter = draw_long_filter(jax.random.fold_in(splits[8], 71), 0)
    skip_gain = jnp.clip(0.5 + 1.0 * jax.random.uniform(splits[6], (MODEL_WIDTH,), jnp.float32) ** level_of(splits[6], (MODEL_WIDTH,), ((0, 8),), -0.2, 0.2), 0.5, 1.5)
    out_weight = centred(splits[7], (MODEL_WIDTH, MODEL_WIDTH), MODEL_WIDTH ** -0.5, 0.09375, ((0, 64), (1, 8)))
    return {"value_in": value_in, "key_in": key_in, "gate_short": gate_short, "gate_long": gate_long, "short_filter": short_filter, "long_filter": long_filter, "skip_gain": skip_gain, "out_weight": out_weight}


def reference(value_in, key_in, gate_short, gate_long, short_filter, long_filter, skip_gain, out_weight):
    product = (value_in.astype(jnp.float32) * key_in.astype(jnp.float32)).astype(jnp.bfloat16)
    tap_table = jnp.repeat(short_filter.astype(jnp.float32), GSIZE, axis=0).T
    padded = jnp.concatenate([jnp.zeros((TAPS - 1, MODEL_WIDTH), jnp.float32), product.astype(jnp.float32)], 0)

    def add_tap(tap_index, total):
        where_at = jnp.asarray(tap_index).astype(jnp.int32)
        start = (TAPS - 1 - where_at).astype(jnp.int32)
        piece = lax.dynamic_slice_in_dim(padded, start, SEQUENCE_TOKENS, 0)
        weights = lax.dynamic_index_in_dim(tap_table, where_at, 0, keepdims=False)
        return total + weights[None, :] * piece

    short_out = lax.fori_loop(0, TAPS, add_tap, jnp.zeros((SEQUENCE_TOKENS, MODEL_WIDTH), jnp.float32))
    mid_rows = (gate_short.astype(jnp.float32) * short_out).astype(jnp.bfloat16)
    span_len = 2 * SEQUENCE_TOKENS
    block_size = min(64, MODEL_WIDTH)

    def block_conv(pair):
        signal, filters = pair
        spectra = jnp.fft.rfft(signal, n=span_len, axis=-1) * jnp.fft.rfft(filters, n=span_len, axis=-1)
        return jnp.fft.irfft(spectra, n=span_len, axis=-1)[:, :SEQUENCE_TOKENS].astype(jnp.float32)

    signals = mid_rows.astype(jnp.float32).T.reshape(MODEL_WIDTH // block_size, block_size, SEQUENCE_TOKENS)
    filters = long_filter.astype(jnp.float32).reshape(MODEL_WIDTH // block_size, block_size, SEQUENCE_TOKENS)
    long_out = lax.map(block_conv, (signals, filters)).reshape(MODEL_WIDTH, SEQUENCE_TOKENS).T.astype(jnp.bfloat16)
    gated = (gate_long.astype(jnp.float32) * (long_out.astype(jnp.float32) + skip_gain.astype(jnp.float32)[None, :] * mid_rows.astype(jnp.float32))).astype(jnp.bfloat16)
    return jnp.dot(gated, out_weight, preferred_element_type=jnp.float32).astype(jnp.bfloat16)
```

```python
import jax
import jax.numpy as jnp
from jax import lax
from jax.experimental import pallas as pl
from jax.experimental.pallas import tpu as pltpu
from jax.sharding import Mesh
from jax.sharding import PartitionSpec as P

CTX = ("x", "zh", "y")
CH = ("zl", "core")
LANES = 128
F32 = jnp.float32
BF16 = jnp.bfloat16


def rolled_rows(row):
    square = jnp.broadcast_to(row, (LANES, LANES))
    return pltpu.roll(square, 0, axis=1, stride=1, stride_axis=0)


def upper():
    rows = lax.broadcasted_iota(jnp.int32, (LANES, LANES), 0)
    cols = lax.broadcasted_iota(jnp.int32, (LANES, LANES), 1)
    return cols >= rows


def band_kernel(taps_ref, band_ref):
    own = upper()
    taps = taps_ref[...].astype(F32)
    for g in range(taps_ref.shape[0]):
        turned = rolled_rows(taps[g : g + 1, :])
        band_ref[g, :LANES, :] = jnp.where(own, 0.0, turned).astype(BF16)
        band_ref[g, LANES:, :] = jnp.where(own, turned, 0.0).astype(BF16)


def short_bands(short_filter):
    groups, taps = short_filter.shape
    return pl.pallas_call(
        band_kernel,
        out_shape=jax.ShapeDtypeStruct((groups, 2 * taps, taps), BF16),
        name="short_bands",
        compiler_params=pltpu.CompilerParams(vmem_limit_bytes=8 << 20),
        cost_estimate=pl.CostEstimate(
            flops=2_000_000_000, bytes_accessed=groups * taps * taps * 4, transcendentals=0
        ),
    )(short_filter)


def short_kernel(prior_ref, own_ref, gate_ref, band_ref, mid_ref):
    groups = band_ref.shape[0]
    channels = own_ref.shape[1]
    size = channels // groups
    for b in range(channels // LANES):
        cols = slice(b * LANES, (b + 1) * LANES)
        prior = prior_ref[:, cols].astype(F32).T.astype(BF16)
        own = own_ref[:, cols].astype(F32).T.astype(BF16)
        gate = gate_ref[:, cols].astype(F32).T
        both = jnp.concatenate([prior, own], axis=1)
        for s in range(LANES // size):
            rows = slice(s * size, (s + 1) * size)
            out = jnp.dot(
                both[rows, :], band_ref[b * (LANES // size) + s], preferred_element_type=F32
            )
            start = b * LANES + s * size
            mid_ref[start : start + size, :] = (gate[rows, :] * out).astype(BF16)


def short_stage(prior, own, gate, band):
    tokens, channels = own.shape
    return pl.pallas_call(
        short_kernel,
        out_shape=jax.ShapeDtypeStruct((channels, tokens), BF16),
        name="short_stage",
        compiler_params=pltpu.CompilerParams(vmem_limit_bytes=16 << 20),
        cost_estimate=pl.CostEstimate(
            flops=1_000_000_000, bytes_accessed=4 << 20, transcendentals=0
        ),
    )(prior, own, gate, band)


def toeplitz_kernel(steps, filt_ref, out_ref, last):
    own = upper()
    q = pl.program_id(0)

    @pl.when(q == 0)
    def _():
        last[...] = jnp.zeros(last.shape, F32)

    for c in range(filt_ref.shape[0]):
        before = last[c]
        for j in range(steps):
            turned = rolled_rows(filt_ref[c : c + 1, j * LANES : (j + 1) * LANES])
            block = jnp.where(own, turned, before).astype(BF16)
            out_ref[c, j * LANES : (j + 1) * LANES, :] = block
            before = turned
        last[c] = before


def long_blocks(long_filter, steps):
    rows, seq = long_filter.shape
    deep, wide = steps * LANES, seq // steps
    return pl.pallas_call(
        lambda *refs: toeplitz_kernel(steps, *refs),
        grid=(wide // LANES,),
        in_specs=[pl.BlockSpec((rows, deep), lambda q: (0, q))],
        out_specs=pl.BlockSpec((rows, deep, LANES), lambda q: (0, 0, q)),
        out_shape=jax.ShapeDtypeStruct((rows, deep, wide), BF16),
        scratch_shapes=[pltpu.VMEM((rows, LANES, LANES), F32)],
        name="long_blocks",
        compiler_params=pltpu.CompilerParams(vmem_limit_bytes=12 << 20),
        cost_estimate=pl.CostEstimate(
            flops=8_000_000_000, bytes_accessed=rows * deep * wide * 2, transcendentals=0
        ),
    )(long_filter)


def conv_kernel(steps, sig_ref, blk_ref, out_ref, sig, acc):
    c = pl.program_id(0)
    count, rows = sig_ref.shape[0], sig_ref.shape[1]

    @pl.when(c == 0)
    def _():
        sig[...] = sig_ref[...].reshape(count * rows, LANES).astype(F32)

    u = sig[pl.ds(c, count, stride=rows), :]
    at = lax.broadcasted_iota(jnp.int32, (count, LANES), 0)
    shifted = [u.astype(BF16)]
    for j in range(1, steps):
        shifted.append(jnp.where(at >= j, pltpu.roll(u, j, axis=0), 0.0).astype(BF16))
    lhs = jnp.concatenate(shifted, axis=1)
    wide = blk_ref.shape[2]
    half = wide // 2
    near = jnp.dot(lhs, blk_ref[0, :, :half], preferred_element_type=F32)
    far = jnp.dot(lhs[: count // 2], blk_ref[0, :, half:], preferred_element_type=F32)
    total = near[:, :LANES]
    for q in range(1, wide // LANES):
        down = q * steps
        if q * LANES < half:
            part = near[: count - down, q * LANES : (q + 1) * LANES]
        else:
            part = far[: count - down, q * LANES - half : (q + 1) * LANES - half]
        total = total + jnp.concatenate([jnp.zeros((down, LANES), F32), part], axis=0)
    acc[pl.ds(c, count, stride=rows), :] = total

    @pl.when(c == rows - 1)
    def _():
        out_ref[...] = acc[...].reshape(count, rows, LANES).astype(BF16)


def long_stage(signal, blocks, steps):
    count, rows, _ = signal.shape
    _, deep, wide = blocks.shape
    return pl.pallas_call(
        lambda *refs: conv_kernel(steps, *refs),
        grid=(rows,),
        in_specs=[
            pl.BlockSpec((count, rows, LANES), lambda c: (0, 0, 0)),
            pl.BlockSpec((1, deep, wide), lambda c: (c, 0, 0)),
        ],
        out_specs=pl.BlockSpec((count, rows, LANES), lambda c: (0, 0, 0)),
        out_shape=jax.ShapeDtypeStruct(signal.shape, BF16),
        scratch_shapes=[
            pltpu.VMEM((count * rows, LANES), F32),
            pltpu.VMEM((count * rows, LANES), F32),
        ],
        name="long_stage",
        compiler_params=pltpu.CompilerParams(vmem_limit_bytes=16 << 20),
        cost_estimate=pl.CostEstimate(
            flops=8_000_000_000, bytes_accessed=rows * deep * wide * 2, transcendentals=0
        ),
    )(signal, blocks)


def gate_kernel(far, near, long_ref, mid_ref, gate_ref, skip_ref, out_ref):
    channels = gate_ref.shape[1]
    tiles = []
    for b in range(channels // LANES):
        rows = slice(b * LANES, (b + 1) * LANES)
        whole = long_ref[rows, :].astype(F32).T
        mid = mid_ref[rows, :].astype(F32).T
        gate = gate_ref[:, rows].astype(F32)
        tiles.append(gate * (whole + skip_ref[:, rows] * mid))
    half = LANES // 2
    low = lax.broadcasted_iota(jnp.int32, tiles[0].shape, 1) < half

    def piece(i, upper_half):
        tile = tiles[i // 2]
        return tile if (i % 2 == 1) == upper_half else pltpu.roll(tile, half, axis=1)

    for y in range(near):
        both = jnp.where(low, piece(y, False), piece(near + y, True)).astype(BF16)
        for copy in range(out_ref.shape[0]):
            out_ref[copy, :, y * LANES : (y + 1) * LANES] = both


def gate_stage(long_rows, mid_rows, gate, skip, copies, near):
    tokens, channels = gate.shape
    return pl.pallas_call(
        lambda *refs: gate_kernel(2, near, *refs),
        out_shape=jax.ShapeDtypeStruct((copies, tokens, channels), BF16),
        name="gate_stage",
        compiler_params=pltpu.CompilerParams(vmem_limit_bytes=16 << 20),
        cost_estimate=pl.CostEstimate(
            flops=1_000_000_000, bytes_accessed=1 << 20, transcendentals=0
        ),
    )(long_rows, mid_rows, gate, skip)


def project_kernel(near, own_ref, other_ref, weight_ref, out_ref, acc):
    k = pl.program_id(0)
    even = lax.axis_index("core") == 0
    total = jnp.zeros(acc.shape, F32)
    own, other = own_ref[0], other_ref[0]
    first = jnp.where(even, own, other)
    second = jnp.where(even, other, own)
    for y in range(near):
        cols = slice(y * LANES, (y + 1) * LANES)
        lhs = jnp.concatenate([first[:, cols], second[:, cols]], axis=1)
        total += jnp.dot(
            lhs, weight_ref[y * 2 * LANES : (y + 1) * 2 * LANES, :], preferred_element_type=F32
        )

    @pl.when(k == 0)
    def _():
        acc[...] = total

    @pl.when(k > 0)
    def _():
        acc[...] += total

    @pl.when(k == pl.num_programs(0) - 1)
    def _():
        out_ref[...] = acc[...].astype(BF16)


def project(own, other, weight, near):
    blocks, tokens, channels = own.shape
    cols = weight.shape[1]
    return pl.pallas_call(
        lambda *refs: project_kernel(near, *refs),
        grid=(blocks,),
        in_specs=[
            pl.BlockSpec((1, tokens, channels), lambda k: (k, 0, 0)),
            pl.BlockSpec((1, tokens, channels), lambda k: (k, 0, 0)),
            pl.BlockSpec((2 * channels, cols), lambda k: (k, 0)),
        ],
        out_specs=pl.BlockSpec((tokens, cols), lambda k: (0, 0)),
        out_shape=jax.ShapeDtypeStruct((tokens, cols), BF16),
        scratch_shapes=[pltpu.VMEM((tokens, cols), F32)],
        name="project",
        compiler_params=pltpu.CompilerParams(vmem_limit_bytes=16 << 20),
    )(own, other, weight)


def next_tokens(value):
    size = lax.axis_size(CTX)
    return lax.ppermute(value, CTX, [(s, s + 1) for s in range(size - 1)])


def in_hbm(value):
    return pltpu.with_memory_space_constraint(value, pltpu.HBM)


def to_each(parts, axes):
    return lax.all_to_all(parts, axes, 0, 0, tiled=True)


def shards(
    value_in, key_in, gate_short, gate_long, short_filter, long_filter, skip_gain, out_weight
):
    tokens, channels = value_in.shape
    ways = lax.axis_size(CTX)
    per_dev = channels // ways
    steps = 8

    product = (value_in.astype(F32) * key_in.astype(F32)).astype(BF16)
    prior = next_tokens(product)
    copies = jnp.broadcast_to(out_weight[None], (lax.axis_size("zh"), *out_weight.shape))
    weight_rows = to_each(copies, "zh").reshape(-1, out_weight.shape[1])
    weight = in_hbm(lax.all_gather(weight_rows, ("x", "y"), axis=0, tiled=True))

    mid = short_stage(prior, product, gate_short, short_bands(short_filter))
    spread = to_each(mid.reshape(ways, per_dev, tokens), CTX)
    blocks = in_hbm(long_blocks(long_filter, steps))
    long_part = long_stage(spread, blocks, steps)
    returned = to_each(long_part, CTX).reshape(channels, tokens)
    near = lax.axis_size("y")
    gated = gate_stage(
        returned, mid, gate_long, skip_gain[None, :], lax.axis_size("zl"), near
    )
    own = to_each(gated, "zl")
    other = lax.ppermute(own, "core", [(0, 1), (1, 0)])
    return project(own, other, weight, near)


def solution(mesh):
    fine = Mesh(mesh.devices.reshape(4, 4, 4, 4, 2), CTX + CH)
    in_specs = (
        P(CTX, CH),
        P(CTX, CH),
        P(CTX, CH),
        P(CTX, CH),
        P(CH, None),
        P(CH + CTX, None),
        P(CH),
        P(CTX, CH),
    )
    return jax.shard_map(
        shards, mesh=fine, in_specs=in_specs, out_specs=P(CTX, CH), check_vma=False
    )
```

```python
import jax
import jax.numpy as jnp
from jax import lax
from jax.experimental import pallas as pl
from jax.experimental.pallas import tpu as pltpu
from jax.sharding import Mesh
from jax.sharding import PartitionSpec as P

CTX = ("x", "zh", "y")
CH = ("zl", "core")
LANES = 128
HALF = LANES // 2
F32 = jnp.float32
BF16 = jnp.bfloat16


def rolled_rows(row, rows=LANES):
    square = jnp.broadcast_to(row, (rows, LANES))
    return pltpu.roll(square, 0, axis=1, stride=1, stride_axis=0)


def upper(rows=LANES):
    at = lax.broadcasted_iota(jnp.int32, (rows, LANES), 0)
    cols = lax.broadcasted_iota(jnp.int32, (rows, LANES), 1)
    return cols >= at


def band_kernel(taps_ref, band_ref):
    own = upper()
    taps = taps_ref[...].astype(F32)
    for g in range(taps_ref.shape[0]):
        turned = rolled_rows(taps[g : g + 1, :])
        band_ref[g, :LANES, :] = jnp.where(own, 0.0, turned).astype(BF16)
        band_ref[g, LANES:, :] = jnp.where(own, turned, 0.0).astype(BF16)


def short_bands(short_filter):
    groups, taps = short_filter.shape
    return pl.pallas_call(
        band_kernel,
        out_shape=jax.ShapeDtypeStruct((groups, 2 * taps, taps), BF16),
        name="short_bands",
        compiler_params=pltpu.CompilerParams(vmem_limit_bytes=8 << 20),
        cost_estimate=pl.CostEstimate(
            flops=2_000_000_000, bytes_accessed=groups * taps * taps * 4, transcendentals=0
        ),
    )(short_filter)


def short_kernel(prior_ref, own_ref, gate_ref, band_ref, mid_ref):
    groups = band_ref.shape[0]
    channels = own_ref.shape[1]
    size = channels // groups
    for b in range(channels // LANES):
        cols = slice(b * LANES, (b + 1) * LANES)
        prior = prior_ref[:, cols].astype(F32).T.astype(BF16)
        own = own_ref[:, cols].astype(F32).T.astype(BF16)
        gate = gate_ref[:, cols].astype(F32).T
        both = jnp.concatenate([prior, own], axis=1)
        for s in range(LANES // size):
            rows = slice(s * size, (s + 1) * size)
            out = jnp.dot(
                both[rows, :], band_ref[b * (LANES // size) + s], preferred_element_type=F32
            )
            start = b * LANES + s * size
            mid_ref[start : start + size, :] = (gate[rows, :] * out).astype(BF16)


def short_stage(prior, own, gate, band):
    tokens, channels = own.shape
    return pl.pallas_call(
        short_kernel,
        out_shape=jax.ShapeDtypeStruct((channels, tokens), BF16),
        name="short_stage",
        compiler_params=pltpu.CompilerParams(vmem_limit_bytes=16 << 20),
        cost_estimate=pl.CostEstimate(
            flops=1_000_000_000, bytes_accessed=4 << 20, transcendentals=0
        ),
    )(prior, own, gate, band)


def toeplitz_kernel(filt_ref, out_ref, last):
    own = upper(HALF)

    @pl.when(pl.program_id(0) == 0)
    def _():
        last[...] = jnp.zeros(last.shape, F32)

    for c in range(filt_ref.shape[0]):
        before = last[c]
        for i in range(filt_ref.shape[1] // LANES):
            cols = slice(i * LANES, (i + 1) * LANES)
            turned = rolled_rows(filt_ref[c : c + 1, cols], HALF)
            out_ref[c, :, cols] = jnp.where(own, turned, before).astype(BF16)
            before = turned
        last[c] = before


def long_blocks(long_filter):
    rows, seq = long_filter.shape
    steps = 8
    wide = seq // steps
    return pl.pallas_call(
        toeplitz_kernel,
        grid=(steps,),
        in_specs=[pl.BlockSpec((rows, wide), lambda j: (0, j))],
        out_specs=pl.BlockSpec((rows, HALF, wide), lambda j: (0, j, 0)),
        out_shape=jax.ShapeDtypeStruct((rows, steps * HALF, wide), BF16),
        scratch_shapes=[pltpu.VMEM((rows, HALF, LANES), F32)],
        name="long_blocks",
        compiler_params=pltpu.CompilerParams(vmem_limit_bytes=58 << 20),
        cost_estimate=pl.CostEstimate(
            flops=4_000_000_000, bytes_accessed=rows * steps * HALF * wide * 2, transcendentals=0
        ),
    )(long_filter)


def moved_down(x, rows):
    if rows == 0:
        return x
    return jnp.concatenate([jnp.zeros((rows, x.shape[1]), x.dtype), x[:-rows]], axis=0)


def turned_down(x, rows, at):
    return x if rows == 0 else jnp.where(at >= rows, pltpu.roll(x, rows, axis=0), 0.0)


def conv_channel(u, blk_ref, i):
    count = u.shape[0]
    at = lax.broadcasted_iota(jnp.int32, u.shape, 0)
    low = lax.broadcasted_iota(jnp.int32, u.shape, 1) < HALF
    w = pltpu.roll(u, HALF, axis=1)
    deep, wide = blk_ref.shape[1:]
    per = wide // (2 * HALF)
    halves = []
    for first, second in ((u, w), (w, u)):
        tiles = [
            jnp.where(low, moved_down(first, per * j), moved_down(second, per * (j + 1)))
            for j in range(0, deep // HALF, 2)
        ]
        halves.append(jnp.concatenate(tiles, axis=1))
    lhs = jnp.concatenate(halves, axis=0).astype(BF16)
    even = jnp.zeros(u.shape, F32)
    odd = jnp.zeros(u.shape, F32)
    for p in range(0, per, 2):
        both = jnp.dot(
            lhs, blk_ref[i, :, p * LANES : (p + 2) * LANES], preferred_element_type=F32
        )
        for k in range(2):
            part = both[:, k * LANES : (k + 1) * LANES]
            even += turned_down(part[:count], p + k, at)
            odd += turned_down(part[count:], p + k, at)
    odd = pltpu.roll(odd, HALF, axis=1)
    return even + jnp.where(low, turned_down(odd, 1, at), odd)


def conv_kernel(sig_ref, blk_ref, out_ref, sig, acc):
    step = pl.program_id(0)
    count, rows = sig_ref.shape[0], sig_ref.shape[1]
    each = blk_ref.shape[0]

    @pl.when(step == 0)
    def _():
        sig[...] = sig_ref[...].reshape(count * rows, LANES).astype(F32)

    for i in range(each):
        at = pl.ds(step * each + i, count, stride=rows)
        acc[at, :] = conv_channel(sig[at, :], blk_ref, i)

    @pl.when(step == pl.num_programs(0) - 1)
    def _():
        out_ref[...] = acc[...].reshape(count, rows, LANES).astype(BF16)


def long_stage(signal, blocks):
    count, rows, _ = signal.shape
    _, deep, wide = blocks.shape
    each = 2
    return pl.pallas_call(
        conv_kernel,
        grid=(rows // each,),
        in_specs=[
            pl.BlockSpec((count, rows, LANES), lambda c: (0, 0, 0)),
            pl.BlockSpec((each, deep, wide), lambda c: (c, 0, 0)),
        ],
        out_specs=pl.BlockSpec((count, rows, LANES), lambda c: (0, 0, 0)),
        out_shape=jax.ShapeDtypeStruct(signal.shape, BF16),
        scratch_shapes=[
            pltpu.VMEM((count * rows, LANES), F32),
            pltpu.VMEM((count * rows, LANES), F32),
        ],
        name="long_stage",
        compiler_params=pltpu.CompilerParams(vmem_limit_bytes=16 << 20),
        cost_estimate=pl.CostEstimate(
            flops=8_000_000_000, bytes_accessed=rows * deep * wide * 2, transcendentals=0
        ),
    )(signal, blocks)


def gate_kernel(near, long_ref, mid_ref, gate_ref, skip_ref, out_ref):
    channels = gate_ref.shape[1]
    tiles = []
    for b in range(channels // LANES):
        rows = slice(b * LANES, (b + 1) * LANES)
        whole = long_ref[rows, :].astype(F32).T
        mid = mid_ref[rows, :].astype(F32).T
        gate = gate_ref[:, rows].astype(F32)
        tiles.append(gate * (whole + skip_ref[:, rows] * mid))
    half = LANES // 2
    low = lax.broadcasted_iota(jnp.int32, tiles[0].shape, 1) < half

    def piece(i, upper_half):
        tile = tiles[i // 2]
        return tile if (i % 2 == 1) == upper_half else pltpu.roll(tile, half, axis=1)

    for y in range(near):
        both = jnp.where(low, piece(y, False), piece(near + y, True)).astype(BF16)
        for copy in range(out_ref.shape[0]):
            out_ref[copy, :, y * LANES : (y + 1) * LANES] = both


def gate_stage(long_rows, mid_rows, gate, skip, copies, near):
    tokens, channels = gate.shape
    return pl.pallas_call(
        lambda *refs: gate_kernel(near, *refs),
        out_shape=jax.ShapeDtypeStruct((copies, tokens, channels), BF16),
        name="gate_stage",
        compiler_params=pltpu.CompilerParams(vmem_limit_bytes=16 << 20),
        cost_estimate=pl.CostEstimate(
            flops=1_000_000_000, bytes_accessed=1 << 20, transcendentals=0
        ),
    )(long_rows, mid_rows, gate, skip)


def project_kernel(near, own_ref, other_ref, weight_ref, out_ref, acc):
    k = pl.program_id(0)
    even = lax.axis_index("core") == 0
    total = jnp.zeros(acc.shape, F32)
    own, other = own_ref[0], other_ref[0]
    first = jnp.where(even, own, other)
    second = jnp.where(even, other, own)
    for y in range(near):
        cols = slice(y * LANES, (y + 1) * LANES)
        lhs = jnp.concatenate([first[:, cols], second[:, cols]], axis=1)
        total += jnp.dot(
            lhs, weight_ref[y * 2 * LANES : (y + 1) * 2 * LANES, :], preferred_element_type=F32
        )

    @pl.when(k == 0)
    def _():
        acc[...] = total

    @pl.when(k > 0)
    def _():
        acc[...] += total

    @pl.when(k == pl.num_programs(0) - 1)
    def _():
        out_ref[...] = acc[...].astype(BF16)


def project(own, other, weight, near):
    blocks, tokens, channels = own.shape
    cols = weight.shape[1]
    return pl.pallas_call(
        lambda *refs: project_kernel(near, *refs),
        grid=(blocks,),
        in_specs=[
            pl.BlockSpec((1, tokens, channels), lambda k: (k, 0, 0)),
            pl.BlockSpec((1, tokens, channels), lambda k: (k, 0, 0)),
            pl.BlockSpec((2 * channels, cols), lambda k: (k, 0)),
        ],
        out_specs=pl.BlockSpec((tokens, cols), lambda k: (0, 0)),
        out_shape=jax.ShapeDtypeStruct((tokens, cols), BF16),
        scratch_shapes=[pltpu.VMEM((tokens, cols), F32)],
        name="project",
        compiler_params=pltpu.CompilerParams(vmem_limit_bytes=16 << 20),
    )(own, other, weight)


def next_tokens(value):
    size = lax.axis_size(CTX)
    return lax.ppermute(value, CTX, [(s, s + 1) for s in range(size - 1)])


def in_hbm(value):
    return pltpu.with_memory_space_constraint(value, pltpu.HBM)


def to_each(parts, axes):
    return lax.all_to_all(parts, axes, 0, 0, tiled=True)


def shards(
    value_in, key_in, gate_short, gate_long, short_filter, long_filter, skip_gain, out_weight
):
    tokens, channels = value_in.shape
    ways = lax.axis_size(CTX)
    per_dev = channels // ways
    near = lax.axis_size("y")

    copies = jnp.broadcast_to(out_weight[None], (lax.axis_size("zh"), *out_weight.shape))
    weight_rows = to_each(copies, "zh").reshape(-1, out_weight.shape[1])
    weight = in_hbm(lax.all_gather(weight_rows, ("x", "y"), axis=0, tiled=True))
    product = (value_in.astype(F32) * key_in.astype(F32)).astype(BF16)
    prior = next_tokens(product)
    bands = short_bands(short_filter)
    mid = short_stage(prior, product, gate_short, bands)
    spread = to_each(mid.reshape(ways, per_dev, tokens), CTX)
    blocks = in_hbm(long_blocks(long_filter))
    long_part = long_stage(spread, blocks)
    returned = to_each(long_part, CTX).reshape(channels, tokens)
    gated = gate_stage(returned, mid, gate_long, skip_gain[None, :], lax.axis_size("zl"), near)
    own = to_each(gated, "zl")
    other = lax.ppermute(own, "core", [(0, 1), (1, 0)])
    return project(own, other, weight, near)


def solution(mesh):
    fine = Mesh(mesh.devices.reshape(4, 4, 4, 4, 2), CTX + CH)
    in_specs = (
        P(CTX, CH),
        P(CTX, CH),
        P(CTX, CH),
        P(CTX, CH),
        P(CH, None),
        P(CH + CTX, None),
        P(CH),
        P(CTX, CH),
    )
    return jax.shard_map(
        shards, mesh=fine, in_specs=in_specs, out_specs=P(CTX, CH), check_vma=False
    )
```

```python
import jax
import jax.numpy as jnp
from jax import lax
from jax.experimental import pallas as pl
from jax.experimental.pallas import tpu as pltpu
from jax.sharding import Mesh
from jax.sharding import PartitionSpec as P

CTX = ("x", "zh", "y")
CH = ("zl", "core")
LANES = 128
HALF = LANES // 2
F32 = jnp.float32
BF16 = jnp.bfloat16


def rolled_rows(row, rows=LANES):
    square = jnp.broadcast_to(row, (rows, LANES))
    return pltpu.roll(square, 0, axis=1, stride=1, stride_axis=0)


def upper(rows=LANES):
    at = lax.broadcasted_iota(jnp.int32, (rows, LANES), 0)
    cols = lax.broadcasted_iota(jnp.int32, (rows, LANES), 1)
    return cols >= at


def band_kernel(taps_ref, band_ref):
    own = upper()
    taps = taps_ref[...].astype(F32)
    for g in range(taps_ref.shape[0]):
        turned = rolled_rows(taps[g : g + 1, :])
        band_ref[g, :LANES, :] = jnp.where(own, 0.0, turned).astype(BF16)
        band_ref[g, LANES:, :] = jnp.where(own, turned, 0.0).astype(BF16)


def short_bands(short_filter):
    groups, taps = short_filter.shape
    return pl.pallas_call(
        band_kernel,
        out_shape=jax.ShapeDtypeStruct((groups, 2 * taps, taps), BF16),
        name="short_bands",
        compiler_params=pltpu.CompilerParams(vmem_limit_bytes=8 << 20),
        cost_estimate=pl.CostEstimate(
            flops=2_000_000_000, bytes_accessed=groups * taps * taps * 4, transcendentals=0
        ),
    )(short_filter)


def short_kernel(prior_ref, own_ref, gate_ref, band_ref, mid_ref):
    groups = band_ref.shape[0]
    channels = own_ref.shape[1]
    size = channels // groups
    for b in range(channels // LANES):
        cols = slice(b * LANES, (b + 1) * LANES)
        prior = prior_ref[:, cols].astype(F32).T.astype(BF16)
        own = own_ref[:, cols].astype(F32).T.astype(BF16)
        gate = gate_ref[:, cols].astype(F32).T
        both = jnp.concatenate([prior, own], axis=1)
        for s in range(LANES // size):
            rows = slice(s * size, (s + 1) * size)
            out = jnp.dot(
                both[rows, :], band_ref[b * (LANES // size) + s], preferred_element_type=F32
            )
            start = b * LANES + s * size
            mid_ref[start : start + size, :] = (gate[rows, :] * out).astype(BF16)


def short_stage(prior, own, gate, band):
    tokens, channels = own.shape
    return pl.pallas_call(
        short_kernel,
        out_shape=jax.ShapeDtypeStruct((channels, tokens), BF16),
        name="short_stage",
        compiler_params=pltpu.CompilerParams(vmem_limit_bytes=16 << 20),
        cost_estimate=pl.CostEstimate(
            flops=1_000_000_000, bytes_accessed=4 << 20, transcendentals=0
        ),
    )(prior, own, gate, band)


def toeplitz_kernel(filt_ref, out_ref, last):
    own = upper(HALF)

    @pl.when(pl.program_id(0) == 0)
    def _():
        last[...] = jnp.zeros(last.shape, F32)

    for c in range(filt_ref.shape[0]):
        before = last[c]
        for i in range(filt_ref.shape[1] // LANES):
            cols = slice(i * LANES, (i + 1) * LANES)
            turned = rolled_rows(filt_ref[c : c + 1, cols], HALF)
            out_ref[c, :, cols] = jnp.where(own, turned, before).astype(BF16)
            before = turned
        last[c] = before


def long_blocks(long_filter):
    rows, seq = long_filter.shape
    steps = 8
    wide = seq // steps
    return pl.pallas_call(
        toeplitz_kernel,
        grid=(steps,),
        in_specs=[pl.BlockSpec((rows, wide), lambda j: (0, j))],
        out_specs=pl.BlockSpec((rows, HALF, wide), lambda j: (0, j, 0)),
        out_shape=jax.ShapeDtypeStruct((rows, steps * HALF, wide), BF16),
        scratch_shapes=[pltpu.VMEM((rows, HALF, LANES), F32)],
        name="long_blocks",
        compiler_params=pltpu.CompilerParams(vmem_limit_bytes=58 << 20),
        cost_estimate=pl.CostEstimate(
            flops=4_000_000_000, bytes_accessed=rows * steps * HALF * wide * 2, transcendentals=0
        ),
    )(long_filter)


def moved_down(x, rows):
    if rows == 0:
        return x
    return jnp.concatenate([jnp.zeros((rows, x.shape[1]), x.dtype), x[:-rows]], axis=0)


def turned_down(x, rows, at):
    return x if rows == 0 else jnp.where(at >= rows, pltpu.roll(x, rows, axis=0), 0.0)


def conv_channel(u, blk_ref, i):
    count = u.shape[0]
    at = lax.broadcasted_iota(jnp.int32, u.shape, 0)
    low = lax.broadcasted_iota(jnp.int32, u.shape, 1) < HALF
    w = pltpu.roll(u, HALF, axis=1)
    deep, wide = blk_ref.shape[1:]
    per = wide // (2 * HALF)
    halves = []
    for first, second in ((u, w), (w, u)):
        tiles = [
            jnp.where(low, moved_down(first, per * j), moved_down(second, per * (j + 1)))
            for j in range(0, deep // HALF, 2)
        ]
        halves.append(jnp.concatenate(tiles, axis=1))
    lhs = jnp.concatenate(halves, axis=0).astype(BF16)
    even = jnp.zeros(u.shape, F32)
    odd = jnp.zeros(u.shape, F32)
    for p in range(0, per, 2):
        both = jnp.dot(
            lhs, blk_ref[i, :, p * LANES : (p + 2) * LANES], preferred_element_type=F32
        )
        for k in range(2):
            part = both[:, k * LANES : (k + 1) * LANES]
            even += turned_down(part[:count], p + k, at)
            odd += turned_down(part[count:], p + k, at)
    odd = pltpu.roll(odd, HALF, axis=1)
    return even + jnp.where(low, turned_down(odd, 1, at), odd)


def conv_kernel(sig_ref, blk_ref, out_ref, sig, acc):
    step = pl.program_id(0)
    count, rows = sig_ref.shape[0], sig_ref.shape[1]
    each = blk_ref.shape[0]

    @pl.when(step == 0)
    def _():
        sig[...] = sig_ref[...].reshape(count * rows, LANES).astype(F32)

    for i in range(each):
        at = pl.ds(step * each + i, count, stride=rows)
        acc[at, :] = conv_channel(sig[at, :], blk_ref, i)

    @pl.when(step == pl.num_programs(0) - 1)
    def _():
        out_ref[...] = acc[...].reshape(count, rows, LANES).astype(BF16)


def long_stage(signal, blocks):
    count, rows, _ = signal.shape
    _, deep, wide = blocks.shape
    each = 2
    return pl.pallas_call(
        conv_kernel,
        grid=(rows // each,),
        in_specs=[
            pl.BlockSpec((count, rows, LANES), lambda c: (0, 0, 0)),
            pl.BlockSpec((each, deep, wide), lambda c: (c, 0, 0)),
        ],
        out_specs=pl.BlockSpec((count, rows, LANES), lambda c: (0, 0, 0)),
        out_shape=jax.ShapeDtypeStruct(signal.shape, BF16),
        scratch_shapes=[
            pltpu.VMEM((count * rows, LANES), F32),
            pltpu.VMEM((count * rows, LANES), F32),
        ],
        name="long_stage",
        compiler_params=pltpu.CompilerParams(vmem_limit_bytes=16 << 20),
        cost_estimate=pl.CostEstimate(
            flops=8_000_000_000, bytes_accessed=rows * deep * wide * 2, transcendentals=0
        ),
    )(signal, blocks)


def gate_kernel(near, long_ref, mid_ref, gate_ref, skip_ref, out_ref):
    channels = gate_ref.shape[1]
    tiles = []
    for b in range(channels // LANES):
        rows = slice(b * LANES, (b + 1) * LANES)
        whole = long_ref[rows, :].astype(F32).T
        mid = mid_ref[rows, :].astype(F32).T
        gate = gate_ref[:, rows].astype(F32)
        tiles.append(gate * (whole + skip_ref[:, rows] * mid))
    half = LANES // 2
    low = lax.broadcasted_iota(jnp.int32, tiles[0].shape, 1) < half

    def piece(i, upper_half):
        tile = tiles[i // 2]
        return tile if (i % 2 == 1) == upper_half else pltpu.roll(tile, half, axis=1)

    for y in range(near):
        both = jnp.where(low, piece(y, False), piece(near + y, True)).astype(BF16)
        for copy in range(out_ref.shape[0]):
            out_ref[copy, :, y * LANES : (y + 1) * LANES] = both


def gate_stage(long_rows, mid_rows, gate, skip, copies, near):
    tokens, channels = gate.shape
    return pl.pallas_call(
        lambda *refs: gate_kernel(near, *refs),
        out_shape=jax.ShapeDtypeStruct((copies, tokens, channels), BF16),
        name="gate_stage",
        compiler_params=pltpu.CompilerParams(vmem_limit_bytes=16 << 20),
        cost_estimate=pl.CostEstimate(
            flops=1_000_000_000, bytes_accessed=1 << 20, transcendentals=0
        ),
    )(long_rows, mid_rows, gate, skip)


def project_kernel(core_ref, *refs):
    feature_ref, weight_ref, before_ref, out_ref, acc = refs
    k = pl.program_id(0)
    rows = weight_ref.shape[1] * weight_ref.shape[3]
    weight = weight_ref[...].reshape(rows, weight_ref.shape[4])
    part = jnp.dot(feature_ref[0], weight, preferred_element_type=F32)

    @pl.when(k == 0)
    def _():
        acc[...] = part if before_ref is None else before_ref[...] + part

    @pl.when(k > 0)
    def _():
        acc[...] += part

    @pl.when(k == pl.num_programs(0) - 1)
    def _():
        out_ref[...] = acc[...].astype(out_ref.dtype)


def project(features, weight, core, before, near):
    blocks, tokens, channels = features.shape
    cols = weight.shape[1]
    parts = in_hbm(weight.reshape(blocks, near, 2, channels // near, cols))
    in_specs = [
        pl.BlockSpec((1, tokens, channels), lambda k, core: (k, 0, 0)),
        pl.BlockSpec((1, near, 1, channels // near, cols), lambda k, core: (k, 0, core[0], 0, 0)),
    ]
    if before is None:
        body = lambda c, f, w, o, acc: project_kernel(c, f, w, None, o, acc)
        more = ()
    else:
        body = project_kernel
        more = (before,)
        in_specs.append(pl.BlockSpec((tokens, cols), lambda k, core: (0, 0)))
    return pl.pallas_call(
        body,
        grid_spec=pltpu.PrefetchScalarGridSpec(
            num_scalar_prefetch=1,
            grid=(blocks,),
            in_specs=in_specs,
            out_specs=pl.BlockSpec((tokens, cols), lambda k, core: (0, 0)),
            scratch_shapes=[pltpu.VMEM((tokens, cols), F32)],
        ),
        out_shape=jax.ShapeDtypeStruct((tokens, cols), F32 if before is None else BF16),
        name="project",
        compiler_params=pltpu.CompilerParams(vmem_limit_bytes=16 << 20),
        cost_estimate=pl.CostEstimate(
            flops=4_000_000_000, bytes_accessed=weight.size, transcendentals=0
        ),
    )(core, features, parts, *more)


def next_tokens(value):
    size = lax.axis_size(CTX)
    return lax.ppermute(value, CTX, [(s, s + 1) for s in range(size - 1)])


def in_hbm(value):
    return pltpu.with_memory_space_constraint(value, pltpu.HBM)


def to_each(parts, axes):
    return lax.all_to_all(parts, axes, 0, 0, tiled=True)


def shards(
    value_in, key_in, gate_short, gate_long, short_filter, long_filter, skip_gain, out_weight
):
    tokens, channels = value_in.shape
    ways = lax.axis_size(CTX)
    per_dev = channels // ways
    near = lax.axis_size("y")

    copies = jnp.broadcast_to(out_weight[None], (lax.axis_size("zh"), *out_weight.shape))
    weight_rows = to_each(copies, "zh").reshape(-1, out_weight.shape[1])
    weight = lax.all_gather(weight_rows, ("x", "y"), axis=0, tiled=True)
    product = (value_in.astype(F32) * key_in.astype(F32)).astype(BF16)
    prior = next_tokens(product)
    bands = short_bands(short_filter)
    mid = short_stage(prior, product, gate_short, bands)
    spread = to_each(mid.reshape(ways, per_dev, tokens), CTX)
    blocks = in_hbm(long_blocks(long_filter))
    long_part = long_stage(spread, blocks)
    returned = to_each(long_part, CTX).reshape(channels, tokens)
    gated = gate_stage(returned, mid, gate_long, skip_gain[None, :], lax.axis_size("zl"), near)
    own = to_each(gated, "zl")
    other = lax.ppermute(own, "core", [(0, 1), (1, 0)])
    core = lax.axis_index("core").reshape(1)
    half = project(own, weight, core, None, near)
    return project(other, weight, 1 - core, half, near)


def solution(mesh):
    fine = Mesh(mesh.devices.reshape(4, 4, 4, 4, 2), CTX + CH)
    in_specs = (
        P(CTX, CH),
        P(CTX, CH),
        P(CTX, CH),
        P(CTX, CH),
        P(CH, None),
        P(CH + CTX, None),
        P(CH),
        P(CTX, CH),
    )
    return jax.shard_map(
        shards, mesh=fine, in_specs=in_specs, out_specs=P(CTX, CH), check_vma=False
    )
```

```python
import jax
import jax.numpy as jnp
from jax import lax
from jax.experimental import pallas as pl
from jax.experimental.pallas import tpu as pltpu
from jax.sharding import Mesh
from jax.sharding import PartitionSpec as P

CTX = ("x", "zh", "y")
CH = ("zl", "core")
LANES = 128
HALF = LANES // 2
F32 = jnp.float32
BF16 = jnp.bfloat16


def rolled_rows(row, rows=LANES):
    square = jnp.broadcast_to(row, (rows, LANES))
    return pltpu.roll(square, 0, axis=1, stride=1, stride_axis=0)


def upper(rows=LANES):
    at = lax.broadcasted_iota(jnp.int32, (rows, LANES), 0)
    cols = lax.broadcasted_iota(jnp.int32, (rows, LANES), 1)
    return cols >= at


def band_kernel(taps_ref, band_ref):
    own = upper()
    taps = taps_ref[...].astype(F32)
    for g in range(taps_ref.shape[0]):
        turned = rolled_rows(taps[g : g + 1, :])
        band_ref[g, :LANES, :] = jnp.where(own, 0.0, turned).astype(BF16)
        band_ref[g, LANES:, :] = jnp.where(own, turned, 0.0).astype(BF16)


def short_bands(short_filter):
    groups, taps = short_filter.shape
    return pl.pallas_call(
        band_kernel,
        out_shape=jax.ShapeDtypeStruct((groups, 2 * taps, taps), BF16),
        name="short_bands",
        compiler_params=pltpu.CompilerParams(vmem_limit_bytes=8 << 20),
        cost_estimate=pl.CostEstimate(
            flops=2_000_000_000, bytes_accessed=groups * taps * taps * 4, transcendentals=0
        ),
    )(short_filter)


def short_kernel(prior_ref, own_ref, gate_ref, band_ref, mid_ref):
    groups = band_ref.shape[0]
    channels = own_ref.shape[1]
    size = channels // groups
    for b in range(channels // LANES):
        cols = slice(b * LANES, (b + 1) * LANES)
        prior = prior_ref[:, cols].astype(F32).T.astype(BF16)
        own = own_ref[:, cols].astype(F32).T.astype(BF16)
        gate = gate_ref[:, cols].astype(F32).T
        both = jnp.concatenate([prior, own], axis=1)
        for s in range(LANES // size):
            rows = slice(s * size, (s + 1) * size)
            out = jnp.dot(
                both[rows, :], band_ref[b * (LANES // size) + s], preferred_element_type=F32
            )
            start = b * LANES + s * size
            mid_ref[start : start + size, :] = (gate[rows, :] * out).astype(BF16)


def short_stage(prior, own, gate, band):
    tokens, channels = own.shape
    return pl.pallas_call(
        short_kernel,
        out_shape=jax.ShapeDtypeStruct((channels, tokens), BF16),
        name="short_stage",
        compiler_params=pltpu.CompilerParams(vmem_limit_bytes=16 << 20),
        cost_estimate=pl.CostEstimate(
            flops=1_000_000_000, bytes_accessed=4 << 20, transcendentals=0
        ),
    )(prior, own, gate, band)


def toeplitz_kernel(filt_ref, after_ref, out_ref, last):
    own = upper(HALF)

    @pl.when(pl.program_id(0) == 0)
    def _():
        last[...] = jnp.zeros(last.shape, F32)

    for c in range(filt_ref.shape[0]):
        before = last[c]
        for i in range(filt_ref.shape[1] // LANES):
            cols = slice(i * LANES, (i + 1) * LANES)
            turned = rolled_rows(filt_ref[c : c + 1, cols], HALF)
            out_ref[c, :, cols] = jnp.where(own, turned, before).astype(BF16)
            before = turned
        last[c] = before


def long_blocks(long_filter, after):
    rows, seq = long_filter.shape
    steps = 8
    wide = seq // steps
    return pl.pallas_call(
        toeplitz_kernel,
        grid=(steps,),
        in_specs=[
            pl.BlockSpec((rows, wide), lambda j: (0, j)),
            pl.BlockSpec(memory_space=pl.ANY),
        ],
        out_specs=pl.BlockSpec((rows, HALF, wide), lambda j: (0, j, 0)),
        out_shape=jax.ShapeDtypeStruct((rows, steps * HALF, wide), BF16),
        scratch_shapes=[pltpu.VMEM((rows, HALF, LANES), F32)],
        name="long_blocks",
        compiler_params=pltpu.CompilerParams(vmem_limit_bytes=58 << 20),
        cost_estimate=pl.CostEstimate(
            flops=4_000_000_000, bytes_accessed=rows * steps * HALF * wide * 2, transcendentals=0
        ),
    )(long_filter, after)


def moved_down(x, rows):
    if rows == 0:
        return x
    return jnp.concatenate([jnp.zeros((rows, x.shape[1]), x.dtype), x[:-rows]], axis=0)


def turned_down(x, rows, at):
    return x if rows == 0 else jnp.where(at >= rows, pltpu.roll(x, rows, axis=0), 0.0)


def conv_channel(u, blk_ref, i):
    count = u.shape[0]
    at = lax.broadcasted_iota(jnp.int32, u.shape, 0)
    low = lax.broadcasted_iota(jnp.int32, u.shape, 1) < HALF
    w = pltpu.roll(u, HALF, axis=1)
    deep, wide = blk_ref.shape[1:]
    per = wide // (2 * HALF)
    halves = []
    for first, second in ((u, w), (w, u)):
        tiles = [
            jnp.where(low, moved_down(first, per * j), moved_down(second, per * (j + 1)))
            for j in range(0, deep // HALF, 2)
        ]
        halves.append(jnp.concatenate(tiles, axis=1))
    lhs = jnp.concatenate(halves, axis=0).astype(BF16)
    even = jnp.zeros(u.shape, F32)
    odd = jnp.zeros(u.shape, F32)
    for p in range(0, per, 2):
        both = jnp.dot(
            lhs, blk_ref[i, :, p * LANES : (p + 2) * LANES], preferred_element_type=F32
        )
        for k in range(2):
            part = both[:, k * LANES : (k + 1) * LANES]
            even += turned_down(part[:count], p + k, at)
            odd += turned_down(part[count:], p + k, at)
    odd = pltpu.roll(odd, HALF, axis=1)
    return even + jnp.where(low, turned_down(odd, 1, at), odd)


def conv_kernel(sig_ref, blk_ref, out_ref, sig, acc):
    step = pl.program_id(0)
    count, rows = sig_ref.shape[0], sig_ref.shape[1]
    each = blk_ref.shape[0]

    @pl.when(step == 0)
    def _():
        sig[...] = sig_ref[...].reshape(count * rows, LANES).astype(F32)

    for i in range(each):
        at = pl.ds(step * each + i, count, stride=rows)
        acc[at, :] = conv_channel(sig[at, :], blk_ref, i)

    @pl.when(step == pl.num_programs(0) - 1)
    def _():
        out_ref[...] = acc[...].reshape(count, rows, LANES).astype(BF16)


def long_stage(signal, blocks):
    count, rows, _ = signal.shape
    _, deep, wide = blocks.shape
    each = 2
    return pl.pallas_call(
        conv_kernel,
        grid=(rows // each,),
        in_specs=[
            pl.BlockSpec((count, rows, LANES), lambda c: (0, 0, 0)),
            pl.BlockSpec((each, deep, wide), lambda c: (c, 0, 0)),
        ],
        out_specs=pl.BlockSpec((count, rows, LANES), lambda c: (0, 0, 0)),
        out_shape=jax.ShapeDtypeStruct(signal.shape, BF16),
        scratch_shapes=[
            pltpu.VMEM((count * rows, LANES), F32),
            pltpu.VMEM((count * rows, LANES), F32),
        ],
        name="long_stage",
        compiler_params=pltpu.CompilerParams(vmem_limit_bytes=16 << 20),
        cost_estimate=pl.CostEstimate(
            flops=8_000_000_000, bytes_accessed=rows * deep * wide * 2, transcendentals=0
        ),
    )(signal, blocks)


def gate_kernel(near, long_ref, mid_ref, gate_ref, skip_ref, out_ref):
    channels = gate_ref.shape[1]
    tiles = []
    for b in range(channels // LANES):
        rows = slice(b * LANES, (b + 1) * LANES)
        whole = long_ref[rows, :].astype(F32).T
        mid = mid_ref[rows, :].astype(F32).T
        gate = gate_ref[:, rows].astype(F32)
        tiles.append(gate * (whole + skip_ref[:, rows] * mid))
    half = LANES // 2
    low = lax.broadcasted_iota(jnp.int32, tiles[0].shape, 1) < half

    def piece(i, upper_half):
        tile = tiles[i // 2]
        return tile if (i % 2 == 1) == upper_half else pltpu.roll(tile, half, axis=1)

    for y in range(near):
        both = jnp.where(low, piece(y, False), piece(near + y, True)).astype(BF16)
        for copy in range(out_ref.shape[0]):
            out_ref[copy, :, y * LANES : (y + 1) * LANES] = both


def gate_stage(long_rows, mid_rows, gate, skip, copies, near):
    tokens, channels = gate.shape
    return pl.pallas_call(
        lambda *refs: gate_kernel(near, *refs),
        out_shape=jax.ShapeDtypeStruct((copies, tokens, channels), BF16),
        name="gate_stage",
        compiler_params=pltpu.CompilerParams(vmem_limit_bytes=16 << 20),
        cost_estimate=pl.CostEstimate(
            flops=1_000_000_000, bytes_accessed=1 << 20, transcendentals=0
        ),
    )(long_rows, mid_rows, gate, skip)


def project_kernel(core_ref, *refs):
    feature_ref, weight_ref, before_ref, out_ref, acc = refs
    k = pl.program_id(0)
    rows = weight_ref.shape[1] * weight_ref.shape[3]
    weight = weight_ref[...].reshape(rows, weight_ref.shape[4])
    part = jnp.dot(feature_ref[0], weight, preferred_element_type=F32)

    @pl.when(k == 0)
    def _():
        acc[...] = part if before_ref is None else before_ref[...] + part

    @pl.when(k > 0)
    def _():
        acc[...] += part

    @pl.when(k == pl.num_programs(0) - 1)
    def _():
        out_ref[...] = acc[...].astype(out_ref.dtype)


def project(features, weight, core, before, near):
    blocks, tokens, channels = features.shape
    cols = weight.shape[1]
    parts = in_hbm(weight.reshape(blocks, near, 2, channels // near, cols))
    in_specs = [
        pl.BlockSpec((1, tokens, channels), lambda k, core: (k, 0, 0)),
        pl.BlockSpec((1, near, 1, channels // near, cols), lambda k, core: (k, 0, core[0], 0, 0)),
    ]
    if before is None:
        body = lambda c, f, w, o, acc: project_kernel(c, f, w, None, o, acc)
        more = ()
    else:
        body = project_kernel
        more = (before,)
        in_specs.append(pl.BlockSpec((tokens, cols), lambda k, core: (0, 0)))
    return pl.pallas_call(
        body,
        grid_spec=pltpu.PrefetchScalarGridSpec(
            num_scalar_prefetch=1,
            grid=(blocks,),
            in_specs=in_specs,
            out_specs=pl.BlockSpec((tokens, cols), lambda k, core: (0, 0)),
            scratch_shapes=[pltpu.VMEM((tokens, cols), F32)],
        ),
        out_shape=jax.ShapeDtypeStruct((tokens, cols), F32 if before is None else BF16),
        name="project",
        compiler_params=pltpu.CompilerParams(vmem_limit_bytes=16 << 20),
        cost_estimate=pl.CostEstimate(
            flops=4_000_000_000, bytes_accessed=weight.size, transcendentals=0
        ),
    )(core, features, parts, *more)


def placed_kernel(*refs):
    *value_refs, out_ref, mark_ref, sems = refs
    me = lax.axis_index("zh")
    size = len(value_refs)
    copies = [
        pltpu.make_async_copy(ref, out_ref.at[lax.rem(me + size - k, size)], sems.at[k])
        for k, ref in enumerate(value_refs)
    ]
    for copy in copies:
        copy.start()
    mark_ref[...] = jnp.zeros(mark_ref.shape, F32)
    for copy in copies:
        copy.wait()


def placed(values):
    shape = values[0].shape
    return pl.pallas_call(
        placed_kernel,
        out_shape=(
            jax.ShapeDtypeStruct((len(values), *shape), values[0].dtype),
            jax.ShapeDtypeStruct((8, LANES), F32),
        ),
        in_specs=[pl.BlockSpec(memory_space=pltpu.VMEM)] * len(values),
        out_specs=(
            pl.BlockSpec(memory_space=pltpu.HBM),
            pl.BlockSpec(memory_space=pltpu.VMEM),
        ),
        scratch_shapes=[pltpu.SemaphoreType.DMA((len(values),))],
        name="placed",
        compiler_params=pltpu.CompilerParams(vmem_limit_bytes=4 << 20),
        cost_estimate=pl.CostEstimate(
            flops=100_000_000, bytes_accessed=values[0].size * 16, transcendentals=0
        ),
    )(*values)


def passed_round(value, axis, steps):
    size = lax.axis_size(axis)
    return lax.ppermute(value, axis, [(s, (s + steps) % size) for s in range(size)])


def next_tokens(value):
    size = lax.axis_size(CTX)
    return lax.ppermute(value, CTX, [(s, s + 1) for s in range(size - 1)])


def in_hbm(value):
    return pltpu.with_memory_space_constraint(value, pltpu.HBM)


def to_each(parts, axes):
    return lax.all_to_all(parts, axes, 0, 0, tiled=True)


def shards(
    value_in, key_in, gate_short, gate_long, short_filter, long_filter, skip_gain, out_weight
):
    tokens, channels = value_in.shape
    ways = lax.axis_size(CTX)
    per_dev = channels // ways
    near = lax.axis_size("y")

    far2 = passed_round(out_weight, "zh", 2)
    far1 = passed_round(out_weight, "zh", 1)
    far3 = passed_round(out_weight, "zh", 3)
    weight_rows, mark = placed([out_weight, far1, far2, far3])
    weight_rows = weight_rows.reshape(-1, out_weight.shape[1])
    weight = lax.all_gather(weight_rows, ("x", "y"), axis=0, tiled=True)
    product = (value_in.astype(F32) * key_in.astype(F32)).astype(BF16)
    prior = next_tokens(product)
    bands = short_bands(short_filter)
    mid = short_stage(prior, product, gate_short, bands)
    spread = to_each(mid.reshape(ways, per_dev, tokens), CTX)
    blocks = in_hbm(long_blocks(long_filter, mark))
    long_part = long_stage(spread, blocks)
    returned = to_each(long_part, CTX).reshape(channels, tokens)
    gated = gate_stage(returned, mid, gate_long, skip_gain[None, :], lax.axis_size("zl"), near)
    own = to_each(gated, "zl")
    other = lax.ppermute(own, "core", [(0, 1), (1, 0)])
    core = lax.axis_index("core").reshape(1)
    half = project(own, weight, core, None, near)
    return project(other, weight, 1 - core, half, near)


def solution(mesh):
    fine = Mesh(mesh.devices.reshape(4, 4, 4, 4, 2), CTX + CH)
    in_specs = (
        P(CTX, CH),
        P(CTX, CH),
        P(CTX, CH),
        P(CTX, CH),
        P(CH, None),
        P(CH + CTX, None),
        P(CH),
        P(CTX, CH),
    )
    return jax.shard_map(
        shards, mesh=fine, in_specs=in_specs, out_specs=P(CTX, CH), check_vma=False
    )
```

```python
import jax
import jax.numpy as jnp
from jax import lax
from jax.experimental import pallas as pl
from jax.experimental.pallas import tpu as pltpu
from jax.sharding import Mesh
from jax.sharding import PartitionSpec as P

CTX = ("x", "zh", "y")
CH = ("zl", "core")
LANES = 128
HALF = LANES // 2
F32 = jnp.float32
BF16 = jnp.bfloat16


def rolled_rows(row, rows=LANES):
    square = jnp.broadcast_to(row, (rows, LANES))
    return pltpu.roll(square, 0, axis=1, stride=1, stride_axis=0)


def upper(rows=LANES):
    at = lax.broadcasted_iota(jnp.int32, (rows, LANES), 0)
    cols = lax.broadcasted_iota(jnp.int32, (rows, LANES), 1)
    return cols >= at


def front_kernel(value_hbm, key_hbm, weight_hbm, product_ref, copies_ref, value, key, weight, sems):
    loads = [
        pltpu.make_async_copy(source, target, sems.at[0, k])
        for k, (source, target) in enumerate(
            ((weight_hbm, weight), (value_hbm, value), (key_hbm, key))
        )
    ]
    for load in loads:
        load.start()
    loads[0].wait()
    sends = [
        pltpu.make_async_copy(weight, copies_ref.at[k], sems.at[1, k])
        for k in range(copies_ref.shape[0])
    ]
    for send in sends:
        send.start()
    loads[1].wait()
    loads[2].wait()
    product_ref[...] = (value[...].astype(F32) * key[...].astype(F32)).astype(BF16)
    for send in sends:
        send.wait()


def front(value, key, weight, count):
    hbm = pl.BlockSpec(memory_space=pltpu.HBM)
    return pl.pallas_call(
        front_kernel,
        in_specs=[hbm] * 3,
        out_specs=(pl.BlockSpec(memory_space=pltpu.VMEM), hbm),
        out_shape=(
            jax.ShapeDtypeStruct(value.shape, BF16),
            jax.ShapeDtypeStruct((count, *weight.shape), weight.dtype),
        ),
        scratch_shapes=[
            pltpu.VMEM(value.shape, BF16),
            pltpu.VMEM(key.shape, BF16),
            pltpu.VMEM(weight.shape, weight.dtype),
            pltpu.SemaphoreType.DMA((2, max(count, 3))),
        ],
        name="front",
        compiler_params=pltpu.CompilerParams(vmem_limit_bytes=4 << 20),
    )(in_hbm(value), in_hbm(key), in_hbm(weight))


def band_kernel(taps_ref, band_ref):
    own = upper()
    taps = taps_ref[...].astype(F32)
    for g in range(taps_ref.shape[0]):
        turned = rolled_rows(taps[g : g + 1, :])
        band_ref[g, :LANES, :] = jnp.where(own, 0.0, turned).astype(BF16)
        band_ref[g, LANES:, :] = jnp.where(own, turned, 0.0).astype(BF16)


def short_bands(short_filter):
    groups, taps = short_filter.shape
    return pl.pallas_call(
        band_kernel,
        out_shape=jax.ShapeDtypeStruct((groups, 2 * taps, taps), BF16),
        name="short_bands",
        compiler_params=pltpu.CompilerParams(vmem_limit_bytes=8 << 20),
        cost_estimate=pl.CostEstimate(
            flops=2_000_000_000, bytes_accessed=groups * taps * taps * 4, transcendentals=0
        ),
    )(short_filter)


def short_kernel(prior_ref, own_ref, gate_ref, band_ref, mid_ref):
    groups = band_ref.shape[0]
    channels = own_ref.shape[1]
    size = channels // groups
    for b in range(channels // LANES):
        cols = slice(b * LANES, (b + 1) * LANES)
        prior = prior_ref[:, cols].astype(F32).T.astype(BF16)
        own = own_ref[:, cols].astype(F32).T.astype(BF16)
        gate = gate_ref[:, cols].astype(F32).T
        both = jnp.concatenate([prior, own], axis=1)
        for s in range(LANES // size):
            rows = slice(s * size, (s + 1) * size)
            out = jnp.dot(
                both[rows, :], band_ref[b * (LANES // size) + s], preferred_element_type=F32
            )
            start = b * LANES + s * size
            mid_ref[start : start + size, :] = (gate[rows, :] * out).astype(BF16)


def short_stage(prior, own, gate, band):
    tokens, channels = own.shape
    return pl.pallas_call(
        short_kernel,
        out_shape=jax.ShapeDtypeStruct((channels, tokens), BF16),
        name="short_stage",
        compiler_params=pltpu.CompilerParams(vmem_limit_bytes=16 << 20),
        cost_estimate=pl.CostEstimate(
            flops=1_000_000_000, bytes_accessed=4 << 20, transcendentals=0
        ),
    )(prior, own, gate, band)


def toeplitz_kernel(filt_ref, out_ref, last):
    own = upper(HALF)

    @pl.when(pl.program_id(0) == 0)
    def _():
        last[...] = jnp.zeros(last.shape, F32)

    for c in range(filt_ref.shape[0]):
        before = last[c]
        for i in range(filt_ref.shape[1] // LANES):
            cols = slice(i * LANES, (i + 1) * LANES)
            turned = rolled_rows(filt_ref[c : c + 1, cols], HALF)
            out_ref[c, :, cols] = jnp.where(own, turned, before).astype(BF16)
            before = turned
        last[c] = before


def long_blocks(long_filter):
    rows, seq = long_filter.shape
    steps = 8
    wide = seq // steps
    return pl.pallas_call(
        toeplitz_kernel,
        grid=(steps,),
        in_specs=[pl.BlockSpec((rows, wide), lambda j: (0, j))],
        out_specs=pl.BlockSpec((rows, HALF, wide), lambda j: (0, j, 0)),
        out_shape=jax.ShapeDtypeStruct((rows, steps * HALF, wide), BF16),
        scratch_shapes=[pltpu.VMEM((rows, HALF, LANES), F32)],
        name="long_blocks",
        compiler_params=pltpu.CompilerParams(vmem_limit_bytes=58 << 20),
        cost_estimate=pl.CostEstimate(
            flops=4_000_000_000, bytes_accessed=rows * steps * HALF * wide * 2, transcendentals=0
        ),
    )(long_filter)


def moved_down(x, rows):
    if rows == 0:
        return x
    return jnp.concatenate([jnp.zeros((rows, x.shape[1]), x.dtype), x[:-rows]], axis=0)


def turned_down(x, rows, at):
    return x if rows == 0 else jnp.where(at >= rows, pltpu.roll(x, rows, axis=0), 0.0)


def conv_channel(u, blk_ref, i):
    count = u.shape[0]
    at = lax.broadcasted_iota(jnp.int32, u.shape, 0)
    low = lax.broadcasted_iota(jnp.int32, u.shape, 1) < HALF
    w = pltpu.roll(u, HALF, axis=1)
    deep, wide = blk_ref.shape[1:]
    per = wide // (2 * HALF)
    halves = []
    for first, second in ((u, w), (w, u)):
        tiles = [
            jnp.where(low, moved_down(first, per * j), moved_down(second, per * (j + 1)))
            for j in range(0, deep // HALF, 2)
        ]
        halves.append(jnp.concatenate(tiles, axis=1))
    lhs = jnp.concatenate(halves, axis=0).astype(BF16)
    even = jnp.zeros(u.shape, F32)
    odd = jnp.zeros(u.shape, F32)
    for p in range(0, per, 2):
        both = jnp.dot(
            lhs, blk_ref[i, :, p * LANES : (p + 2) * LANES], preferred_element_type=F32
        )
        for k in range(2):
            part = both[:, k * LANES : (k + 1) * LANES]
            even += turned_down(part[:count], p + k, at)
            odd += turned_down(part[count:], p + k, at)
    odd = pltpu.roll(odd, HALF, axis=1)
    return even + jnp.where(low, turned_down(odd, 1, at), odd)


def conv_kernel(sig_ref, blk_hbm, out_ref, sig, acc, blk, sems):
    count, rows = sig_ref.shape[0], sig_ref.shape[1]
    loads = [pltpu.make_async_copy(blk_hbm.at[c], blk.at[c], sems.at[c]) for c in range(rows)]
    for load in loads:
        load.start()
    sig[...] = sig_ref[...].reshape(count * rows, LANES).astype(F32)
    for c in range(rows):
        at = pl.ds(c, count, stride=rows)
        u = sig[at, :]
        loads[c].wait()
        acc[at, :] = conv_channel(u, blk, c)
    out_ref[...] = acc[...].reshape(count, rows, LANES).astype(BF16)


def long_stage(signal, blocks):
    count, rows, _ = signal.shape
    vmem = pl.BlockSpec(memory_space=pltpu.VMEM)
    return pl.pallas_call(
        conv_kernel,
        in_specs=[vmem, pl.BlockSpec(memory_space=pltpu.HBM)],
        out_specs=vmem,
        out_shape=jax.ShapeDtypeStruct(signal.shape, BF16),
        scratch_shapes=[
            pltpu.VMEM((count * rows, LANES), F32),
            pltpu.VMEM((count * rows, LANES), F32),
            pltpu.VMEM(blocks.shape, BF16),
            pltpu.SemaphoreType.DMA((rows,)),
        ],
        name="long_stage",
        compiler_params=pltpu.CompilerParams(vmem_limit_bytes=24 << 20),
        cost_estimate=pl.CostEstimate(
            flops=8_000_000_000, bytes_accessed=blocks.size * 2, transcendentals=0
        ),
    )(signal, in_hbm(blocks))


def gate_kernel(near, long_ref, mid_ref, gate_ref, skip_ref, out_ref):
    channels = gate_ref.shape[1]
    tiles = []
    for b in range(channels // LANES):
        rows = slice(b * LANES, (b + 1) * LANES)
        whole = long_ref[rows, :].astype(F32).T
        mid = mid_ref[rows, :].astype(F32).T
        gate = gate_ref[:, rows].astype(F32)
        tiles.append(gate * (whole + skip_ref[:, rows] * mid))
    half = LANES // 2
    low = lax.broadcasted_iota(jnp.int32, tiles[0].shape, 1) < half

    def piece(i, upper_half):
        tile = tiles[i // 2]
        return tile if (i % 2 == 1) == upper_half else pltpu.roll(tile, half, axis=1)

    for y in range(near):
        both = jnp.where(low, piece(y, False), piece(near + y, True)).astype(BF16)
        for copy in range(out_ref.shape[0]):
            out_ref[copy, :, y * LANES : (y + 1) * LANES] = both


def gate_stage(long_rows, mid_rows, gate, skip, copies, near):
    tokens, channels = gate.shape
    return pl.pallas_call(
        lambda *refs: gate_kernel(near, *refs),
        out_shape=jax.ShapeDtypeStruct((copies, tokens, channels), BF16),
        name="gate_stage",
        compiler_params=pltpu.CompilerParams(vmem_limit_bytes=16 << 20),
        cost_estimate=pl.CostEstimate(
            flops=1_000_000_000, bytes_accessed=1 << 20, transcendentals=0
        ),
    )(long_rows, mid_rows, gate, skip)


def project_own_kernel(feature_ref, weight_ref, part_ref, rest_ref, held, sems):
    core = lax.axis_index("core")
    blocks = feature_ref.shape[0]
    mine = [
        pltpu.make_async_copy(weight_ref.at[k, :, core], held.at[k], sems.at[0, k])
        for k in range(blocks)
    ]
    rest = [
        pltpu.make_async_copy(weight_ref.at[k, :, 1 - core], rest_ref.at[k], sems.at[1, k])
        for k in range(blocks)
    ]
    for copy in mine + rest:
        copy.start()
    total = jnp.zeros(part_ref.shape, F32)
    for k in range(blocks):
        mine[k].wait()
        weight = held[k].reshape(feature_ref.shape[2], part_ref.shape[1])
        total += jnp.dot(feature_ref[k], weight, preferred_element_type=F32)
    part_ref[...] = total
    for copy in rest:
        copy.wait()


def project_own(features, weight, near):
    blocks, tokens, channels = features.shape
    cols = weight.shape[1]
    parts = in_hbm(weight.reshape(blocks, near, 2, channels // near, cols))
    vmem = pl.BlockSpec(memory_space=pltpu.VMEM)
    half = (blocks, near, channels // near, cols)
    return pl.pallas_call(
        project_own_kernel,
        in_specs=[vmem, pl.BlockSpec(memory_space=pltpu.HBM)],
        out_specs=(vmem, vmem),
        out_shape=(
            jax.ShapeDtypeStruct((tokens, cols), F32),
            jax.ShapeDtypeStruct(half, weight.dtype),
        ),
        scratch_shapes=[
            pltpu.VMEM(half, weight.dtype),
            pltpu.SemaphoreType.DMA((2, blocks)),
        ],
        name="project_own",
        compiler_params=pltpu.CompilerParams(vmem_limit_bytes=8 << 20),
        cost_estimate=pl.CostEstimate(
            flops=4_000_000_000, bytes_accessed=weight.size * 2, transcendentals=0
        ),
    )(features, parts)


def project_other_kernel(feature_ref, weight_ref, part_ref, out_ref):
    total = part_ref[...]
    for k in range(feature_ref.shape[0]):
        weight = weight_ref[k].reshape(feature_ref.shape[2], out_ref.shape[1])
        total += jnp.dot(feature_ref[k], weight, preferred_element_type=F32)
    out_ref[...] = total.astype(BF16)


def project_other(features, weight, part):
    vmem = pl.BlockSpec(memory_space=pltpu.VMEM)
    return pl.pallas_call(
        project_other_kernel,
        in_specs=[vmem] * 3,
        out_specs=vmem,
        out_shape=jax.ShapeDtypeStruct(part.shape, BF16),
        name="project_other",
        compiler_params=pltpu.CompilerParams(vmem_limit_bytes=8 << 20),
    )(features, weight, part)


def next_tokens(value):
    size = lax.axis_size(CTX)
    return lax.ppermute(value, CTX, [(s, s + 1) for s in range(size - 1)])


def in_hbm(value):
    return pltpu.with_memory_space_constraint(value, pltpu.HBM)


def to_each(parts, axes):
    return lax.all_to_all(parts, axes, 0, 0, tiled=True)


def shards(
    value_in, key_in, gate_short, gate_long, short_filter, long_filter, skip_gain, out_weight
):
    tokens, channels = value_in.shape
    ways = lax.axis_size(CTX)
    per_dev = channels // ways
    near = lax.axis_size("y")

    product, copies = front(value_in, key_in, out_weight, lax.axis_size("zh"))
    weight_rows = to_each(copies, "zh").reshape(-1, out_weight.shape[1])
    weight = lax.all_gather(weight_rows, ("x", "y"), axis=0, tiled=True)
    prior = next_tokens(product)
    bands = short_bands(short_filter)
    mid = short_stage(prior, product, gate_short, bands)
    spread = to_each(mid.reshape(ways, per_dev, tokens), CTX)
    blocks = long_blocks(long_filter)
    long_part = long_stage(spread, blocks)
    returned = to_each(long_part, CTX).reshape(channels, tokens)
    gated = gate_stage(returned, mid, gate_long, skip_gain[None, :], lax.axis_size("zl"), near)
    own = to_each(gated, "zl")
    other = lax.ppermute(own, "core", [(0, 1), (1, 0)])
    part, rest = project_own(own, weight, near)
    return project_other(other, rest, part)


def solution(mesh):
    fine = Mesh(mesh.devices.reshape(4, 4, 4, 4, 2), CTX + CH)
    in_specs = (
        P(CTX, CH),
        P(CTX, CH),
        P(CTX, CH),
        P(CTX, CH),
        P(CH, None),
        P(CH + CTX, None),
        P(CH),
        P(CTX, CH),
    )
    return jax.shard_map(
        shards, mesh=fine, in_specs=in_specs, out_specs=P(CTX, CH), check_vma=False
    )
```

```python
import jax
import jax.numpy as jnp
from jax import lax
from jax.experimental import pallas as pl
from jax.experimental.pallas import tpu as pltpu
from jax.sharding import Mesh
from jax.sharding import PartitionSpec as P

CTX = ("x", "zh", "y")
CH = ("zl", "core")
LANES = 128
HALF = LANES // 2
F32 = jnp.float32
BF16 = jnp.bfloat16


def rolled_rows(row, rows=LANES):
    square = jnp.broadcast_to(row, (rows, LANES))
    return pltpu.roll(square, 0, axis=1, stride=1, stride_axis=0)


def upper(rows=LANES):
    at = lax.broadcasted_iota(jnp.int32, (rows, LANES), 0)
    cols = lax.broadcasted_iota(jnp.int32, (rows, LANES), 1)
    return cols >= at


def front_kernel(weight_hbm, copies_ref, weight, sems):
    count = copies_ref.shape[0]
    load = pltpu.make_async_copy(weight_hbm, weight, sems.at[count])
    load.start()
    load.wait()
    sends = [pltpu.make_async_copy(weight, copies_ref.at[k], sems.at[k]) for k in range(count)]
    for send in sends:
        send.start()
    for send in sends:
        send.wait()


def front(weight, count):
    hbm = pl.BlockSpec(memory_space=pltpu.HBM)
    return pl.pallas_call(
        front_kernel,
        in_specs=[hbm],
        out_specs=hbm,
        out_shape=jax.ShapeDtypeStruct((count, *weight.shape), weight.dtype),
        scratch_shapes=[
            pltpu.VMEM(weight.shape, weight.dtype),
            pltpu.SemaphoreType.DMA((count + 1,)),
        ],
        name="front",
        compiler_params=pltpu.CompilerParams(vmem_limit_bytes=4 << 20),
    )(in_hbm(weight))


def pack_kernel(value_ref, key_ref, gate_ref, out_ref):
    rows = out_ref.shape[1] // 2
    peers = LANES // rows
    for b in range(value_ref.shape[1] // LANES):
        cols = slice(b * LANES, (b + 1) * LANES)
        to = slice(b * peers, (b + 1) * peers)
        product = (value_ref[:, cols].astype(F32) * key_ref[:, cols].astype(F32)).astype(BF16)
        out_ref[to, :rows, :] = product.astype(F32).T.reshape(peers, rows, LANES).astype(BF16)
        gate = gate_ref[:, cols].astype(F32).T.reshape(peers, rows, LANES)
        out_ref[to, rows:, :] = gate.astype(BF16)


def pack(value, key, gate, rows):
    tokens, channels = value.shape
    vmem = pl.BlockSpec(memory_space=pltpu.VMEM)
    return pl.pallas_call(
        pack_kernel,
        in_specs=[vmem] * 3,
        out_specs=vmem,
        out_shape=jax.ShapeDtypeStruct((channels // rows, 2 * rows, tokens), BF16),
        name="pack",
        compiler_params=pltpu.CompilerParams(vmem_limit_bytes=16 << 20),
        cost_estimate=pl.CostEstimate(
            flops=1_000_000_000, bytes_accessed=1 << 20, transcendentals=0
        ),
    )(value, key, gate)


def toeplitz_kernel(filt_ref, out_ref, last):
    own = upper(HALF)

    @pl.when(pl.program_id(0) == 0)
    def _():
        last[...] = jnp.zeros(last.shape, F32)

    for c in range(filt_ref.shape[0]):
        before = last[c]
        for i in range(filt_ref.shape[1] // LANES):
            cols = slice(i * LANES, (i + 1) * LANES)
            turned = rolled_rows(filt_ref[c : c + 1, cols], HALF)
            out_ref[c, :, cols] = jnp.where(own, turned, before).astype(BF16)
            before = turned
        last[c] = before


def long_blocks(long_filter):
    rows, seq = long_filter.shape
    steps = 8
    wide = seq // steps
    return pl.pallas_call(
        toeplitz_kernel,
        grid=(steps,),
        in_specs=[pl.BlockSpec((rows, wide), lambda j: (0, j))],
        out_specs=pl.BlockSpec((rows, HALF, wide), lambda j: (0, j, 0)),
        out_shape=jax.ShapeDtypeStruct((rows, steps * HALF, wide), BF16),
        scratch_shapes=[pltpu.VMEM((rows, HALF, LANES), F32)],
        name="long_blocks",
        compiler_params=pltpu.CompilerParams(vmem_limit_bytes=58 << 20),
        cost_estimate=pl.CostEstimate(
            flops=4_000_000_000, bytes_accessed=rows * steps * HALF * wide * 2, transcendentals=0
        ),
    )(long_filter)


def moved_down(x, rows):
    if rows == 0:
        return x
    return jnp.concatenate([jnp.zeros((rows, x.shape[1]), x.dtype), x[:-rows]], axis=0)


def turned_down(x, rows, at):
    return x if rows == 0 else jnp.where(at >= rows, pltpu.roll(x, rows, axis=0), 0.0)


def conv_channel(u, blk_ref, i):
    count = u.shape[0]
    at = lax.broadcasted_iota(jnp.int32, u.shape, 0)
    low = lax.broadcasted_iota(jnp.int32, u.shape, 1) < HALF
    w = pltpu.roll(u, HALF, axis=1)
    deep, wide = blk_ref.shape[1:]
    per = wide // (2 * HALF)
    halves = []
    for first, second in ((u, w), (w, u)):
        tiles = [
            jnp.where(low, moved_down(first, per * j), moved_down(second, per * (j + 1)))
            for j in range(0, deep // HALF, 2)
        ]
        halves.append(jnp.concatenate(tiles, axis=1))
    lhs = jnp.concatenate(halves, axis=0).astype(BF16)
    even = jnp.zeros(u.shape, F32)
    odd = jnp.zeros(u.shape, F32)
    for p in range(0, per, 2):
        both = jnp.dot(
            lhs, blk_ref[i, :, p * LANES : (p + 2) * LANES], preferred_element_type=F32
        )
        for k in range(2):
            part = both[:, k * LANES : (k + 1) * LANES]
            even += turned_down(part[:count], p + k, at)
            odd += turned_down(part[count:], p + k, at)
    odd = pltpu.roll(odd, HALF, axis=1)
    return even + jnp.where(low, turned_down(odd, 1, at), odd)


def ctx_index():
    at = 0
    for axis in CTX:
        at = at * lax.axis_size(axis) + lax.axis_index(axis)
    return at


def conv_kernel(size, sig_ref, taps_ref, skip_ref, blk_hbm, out_ref, sig, acc, blk, sems):
    count, rows = out_ref.shape[0], out_ref.shape[1]
    loads = [pltpu.make_async_copy(blk_hbm.at[c], blk.at[c], sems.at[c]) for c in range(rows)]
    for load in loads:
        load.start()
    me = ctx_index()
    sig[...] = sig_ref[...].reshape(count * 2 * rows, LANES).astype(F32)
    taps = taps_ref[...].astype(F32)
    group = lax.broadcasted_iota(jnp.int32, taps.shape, 0) == me * rows // size
    turned = rolled_rows(jnp.sum(jnp.where(group, taps, 0.0), axis=0, keepdims=True))
    own = upper()
    band = jnp.concatenate([jnp.where(own, 0.0, turned), jnp.where(own, turned, 0.0)], axis=0)
    band = band.astype(BF16)
    at = lax.broadcasted_iota(jnp.int32, (count, LANES), 0)
    lane = lax.broadcasted_iota(jnp.int32, skip_ref.shape, 1)
    for c in range(rows):
        product = sig[pl.ds(c, count, stride=2 * rows), :]
        gate = sig[pl.ds(rows + c, count, stride=2 * rows), :]
        both = jnp.concatenate([turned_down(product, 1, at), product], axis=1).astype(BF16)
        short = jnp.dot(both, band, preferred_element_type=F32)
        mid = (gate * short).astype(BF16).astype(F32)
        loads[c].wait()
        far = conv_channel(mid, blk, c).astype(BF16).astype(F32)
        skip = jnp.sum(
            jnp.where(lane == me * rows + c, skip_ref[...], 0.0), axis=1, keepdims=True
        )
        acc[pl.ds(c, count, stride=rows), :] = far + skip * mid
    out_ref[...] = acc[...].reshape(count, rows, LANES).astype(BF16)


def long_stage(signal, taps, skip, blocks, size):
    count, twice, _ = signal.shape
    rows = twice // 2
    vmem = pl.BlockSpec(memory_space=pltpu.VMEM)
    return pl.pallas_call(
        lambda *refs: conv_kernel(size, *refs),
        in_specs=[vmem, vmem, vmem, pl.BlockSpec(memory_space=pltpu.HBM)],
        out_specs=vmem,
        out_shape=jax.ShapeDtypeStruct((count, rows, LANES), BF16),
        scratch_shapes=[
            pltpu.VMEM((count * twice, LANES), F32),
            pltpu.VMEM((count * rows, LANES), F32),
            pltpu.VMEM(blocks.shape, BF16),
            pltpu.SemaphoreType.DMA((rows,)),
        ],
        name="long_stage",
        compiler_params=pltpu.CompilerParams(vmem_limit_bytes=24 << 20),
        cost_estimate=pl.CostEstimate(
            flops=8_000_000_000, bytes_accessed=blocks.size * 2, transcendentals=0
        ),
    )(signal, taps, skip, in_hbm(blocks))


def gate_kernel(near, long_ref, gate_ref, out_ref):
    channels = gate_ref.shape[1]
    tiles = []
    for b in range(channels // LANES):
        rows = slice(b * LANES, (b + 1) * LANES)
        whole = long_ref[rows, :].astype(F32).T
        gate = gate_ref[:, rows].astype(F32)
        tiles.append(gate * whole)
    half = LANES // 2
    low = lax.broadcasted_iota(jnp.int32, tiles[0].shape, 1) < half

    def piece(i, upper_half):
        tile = tiles[i // 2]
        return tile if (i % 2 == 1) == upper_half else pltpu.roll(tile, half, axis=1)

    for y in range(near):
        both = jnp.where(low, piece(y, False), piece(near + y, True)).astype(BF16)
        for copy in range(out_ref.shape[0]):
            out_ref[copy, :, y * LANES : (y + 1) * LANES] = both


def gate_stage(long_rows, gate, copies, near):
    tokens, channels = gate.shape
    return pl.pallas_call(
        lambda *refs: gate_kernel(near, *refs),
        out_shape=jax.ShapeDtypeStruct((copies, tokens, channels), BF16),
        name="gate_stage",
        compiler_params=pltpu.CompilerParams(vmem_limit_bytes=16 << 20),
        cost_estimate=pl.CostEstimate(
            flops=1_000_000_000, bytes_accessed=1 << 20, transcendentals=0
        ),
    )(long_rows, gate)


def project_own_kernel(feature_ref, weight_ref, part_ref, rest_ref, held, sems):
    core = lax.axis_index("core")
    blocks = feature_ref.shape[0]
    mine = [
        pltpu.make_async_copy(weight_ref.at[k, :, core], held.at[k], sems.at[0, k])
        for k in range(blocks)
    ]
    rest = [
        pltpu.make_async_copy(weight_ref.at[k, :, 1 - core], rest_ref.at[k], sems.at[1, k])
        for k in range(blocks)
    ]
    for copy in mine + rest:
        copy.start()
    total = jnp.zeros(part_ref.shape, F32)
    for k in range(blocks):
        mine[k].wait()
        weight = held[k].reshape(feature_ref.shape[2], part_ref.shape[1])
        total += jnp.dot(feature_ref[k], weight, preferred_element_type=F32)
    part_ref[...] = total
    for copy in rest:
        copy.wait()


def project_own(features, weight, near):
    blocks, tokens, channels = features.shape
    cols = weight.shape[1]
    parts = in_hbm(weight.reshape(blocks, near, 2, channels // near, cols))
    vmem = pl.BlockSpec(memory_space=pltpu.VMEM)
    half = (blocks, near, channels // near, cols)
    return pl.pallas_call(
        project_own_kernel,
        in_specs=[vmem, pl.BlockSpec(memory_space=pltpu.HBM)],
        out_specs=(vmem, vmem),
        out_shape=(
            jax.ShapeDtypeStruct((tokens, cols), F32),
            jax.ShapeDtypeStruct(half, weight.dtype),
        ),
        scratch_shapes=[
            pltpu.VMEM(half, weight.dtype),
            pltpu.SemaphoreType.DMA((2, blocks)),
        ],
        name="project_own",
        compiler_params=pltpu.CompilerParams(vmem_limit_bytes=8 << 20),
        cost_estimate=pl.CostEstimate(
            flops=4_000_000_000, bytes_accessed=weight.size * 2, transcendentals=0
        ),
    )(features, parts)


def project_other_kernel(feature_ref, weight_ref, part_ref, out_ref):
    total = part_ref[...]
    for k in range(feature_ref.shape[0]):
        weight = weight_ref[k].reshape(feature_ref.shape[2], out_ref.shape[1])
        total += jnp.dot(feature_ref[k], weight, preferred_element_type=F32)
    out_ref[...] = total.astype(BF16)


def project_other(features, weight, part):
    vmem = pl.BlockSpec(memory_space=pltpu.VMEM)
    return pl.pallas_call(
        project_other_kernel,
        in_specs=[vmem] * 3,
        out_specs=vmem,
        out_shape=jax.ShapeDtypeStruct(part.shape, BF16),
        name="project_other",
        compiler_params=pltpu.CompilerParams(vmem_limit_bytes=8 << 20),
    )(features, weight, part)


def in_hbm(value):
    return pltpu.with_memory_space_constraint(value, pltpu.HBM)


def to_each(parts, axes):
    return lax.all_to_all(parts, axes, 0, 0, tiled=True)


def shards(
    value_in, key_in, gate_short, gate_long, short_filter, long_filter, skip_gain, out_weight
):
    tokens, channels = value_in.shape
    ways = lax.axis_size(CTX)
    per_dev = channels // ways
    near = lax.axis_size("y")

    copies = front(out_weight, lax.axis_size("zh"))
    weight_rows = to_each(copies, "zh").reshape(-1, out_weight.shape[1])
    weight = lax.all_gather(weight_rows, ("x", "y"), axis=0, tiled=True)
    packed = pack(value_in, key_in, gate_short, per_dev)
    spread = to_each(packed, CTX)
    blocks = long_blocks(long_filter)
    long_part = long_stage(
        spread, short_filter, skip_gain[None, :], blocks, channels // short_filter.shape[0]
    )
    returned = to_each(long_part, CTX).reshape(channels, tokens)
    gated = gate_stage(returned, gate_long, lax.axis_size("zl"), near)
    own = to_each(gated, "zl")
    other = lax.ppermute(own, "core", [(0, 1), (1, 0)])
    part, rest = project_own(own, weight, near)
    return project_other(other, rest, part)


def solution(mesh):
    fine = Mesh(mesh.devices.reshape(4, 4, 4, 4, 2), CTX + CH)
    in_specs = (
        P(CTX, CH),
        P(CTX, CH),
        P(CTX, CH),
        P(CTX, CH),
        P(CH, None),
        P(CH + CTX, None),
        P(CH),
        P(CTX, CH),
    )
    return jax.shard_map(
        shards, mesh=fine, in_specs=in_specs, out_specs=P(CTX, CH), check_vma=False
    )
```

```python
import jax
import jax.numpy as jnp
from jax import lax
from jax.experimental import pallas as pl
from jax.experimental.pallas import tpu as pltpu
from jax.sharding import Mesh
from jax.sharding import PartitionSpec as P

CTX = ("x", "zh", "y")
CH = ("zl", "core")
LANES = 128
HALF = LANES // 2
F32 = jnp.float32
BF16 = jnp.bfloat16


def rolled_rows(row, rows=LANES):
    square = jnp.broadcast_to(row, (rows, LANES))
    return pltpu.roll(square, 0, axis=1, stride=1, stride_axis=0)


def upper(rows=LANES):
    at = lax.broadcasted_iota(jnp.int32, (rows, LANES), 0)
    cols = lax.broadcasted_iota(jnp.int32, (rows, LANES), 1)
    return cols >= at


def pack_kernel(value_hbm, key_hbm, gate_hbm, out_ref, value_ref, key_ref, gate_ref, sems):
    loads = [
        pltpu.make_async_copy(source, target, sems.at[k])
        for k, (source, target) in enumerate(
            ((value_hbm, value_ref), (key_hbm, key_ref), (gate_hbm, gate_ref))
        )
    ]
    for load in loads:
        load.start()
    for load in loads:
        load.wait()
    rows = out_ref.shape[1] // 2
    peers = LANES // rows
    for b in range(value_ref.shape[1] // LANES):
        cols = slice(b * LANES, (b + 1) * LANES)
        to = slice(b * peers, (b + 1) * peers)
        product = (value_ref[:, cols].astype(F32) * key_ref[:, cols].astype(F32)).astype(BF16)
        out_ref[to, :rows, :] = product.astype(F32).T.reshape(peers, rows, LANES).astype(BF16)
        gate = gate_ref[:, cols].astype(F32).T.reshape(peers, rows, LANES)
        out_ref[to, rows:, :] = gate.astype(BF16)


def pack(value, key, gate, rows):
    tokens, channels = value.shape
    return pl.pallas_call(
        pack_kernel,
        in_specs=[pl.BlockSpec(memory_space=pltpu.HBM)] * 3,
        out_specs=pl.BlockSpec(memory_space=pltpu.VMEM),
        scratch_shapes=[pltpu.VMEM(value.shape, BF16)] * 3 + [pltpu.SemaphoreType.DMA((3,))],
        out_shape=jax.ShapeDtypeStruct((channels // rows, 2 * rows, tokens), BF16),
        name="pack",
        compiler_params=pltpu.CompilerParams(vmem_limit_bytes=16 << 20),
        cost_estimate=pl.CostEstimate(
            flops=1_000_000_000, bytes_accessed=1 << 20, transcendentals=0
        ),
    )(in_hbm(value), in_hbm(key), in_hbm(gate))


def toeplitz_kernel(filt_ref, out_ref, last):
    own = upper(HALF)

    @pl.when(pl.program_id(0) == 0)
    def _():
        last[...] = jnp.zeros(last.shape, F32)

    for c in range(filt_ref.shape[0]):
        before = last[c]
        for i in range(filt_ref.shape[1] // LANES):
            cols = slice(i * LANES, (i + 1) * LANES)
            turned = rolled_rows(filt_ref[c : c + 1, cols], HALF)
            out_ref[c, :, cols] = jnp.where(own, turned, before).astype(BF16)
            before = turned
        last[c] = before


def long_blocks(long_filter):
    rows, seq = long_filter.shape
    steps = 8
    wide = seq // steps
    return pl.pallas_call(
        toeplitz_kernel,
        grid=(steps,),
        in_specs=[pl.BlockSpec((rows, wide), lambda j: (0, j))],
        out_specs=pl.BlockSpec((rows, HALF, wide), lambda j: (0, j, 0)),
        out_shape=jax.ShapeDtypeStruct((rows, steps * HALF, wide), BF16),
        scratch_shapes=[pltpu.VMEM((rows, HALF, LANES), F32)],
        name="long_blocks",
        compiler_params=pltpu.CompilerParams(vmem_limit_bytes=58 << 20),
        cost_estimate=pl.CostEstimate(
            flops=4_000_000_000, bytes_accessed=rows * steps * HALF * wide * 2, transcendentals=0
        ),
    )(long_filter)


def moved_down(x, rows):
    if rows == 0:
        return x
    return jnp.concatenate([jnp.zeros((rows, x.shape[1]), x.dtype), x[:-rows]], axis=0)


def turned_down(x, rows, at):
    return x if rows == 0 else jnp.where(at >= rows, pltpu.roll(x, rows, axis=0), 0.0)


def conv_channel(u, blk_ref, i):
    count = u.shape[0]
    at = lax.broadcasted_iota(jnp.int32, u.shape, 0)
    low = lax.broadcasted_iota(jnp.int32, u.shape, 1) < HALF
    w = pltpu.roll(u, HALF, axis=1)
    deep, wide = blk_ref.shape[1:]
    per = wide // (2 * HALF)
    halves = []
    for first, second in ((u, w), (w, u)):
        tiles = [
            jnp.where(low, moved_down(first, per * j), moved_down(second, per * (j + 1)))
            for j in range(0, deep // HALF, 2)
        ]
        halves.append(jnp.concatenate(tiles, axis=1))
    lhs = jnp.concatenate(halves, axis=0).astype(BF16)
    even = jnp.zeros(u.shape, F32)
    odd = jnp.zeros(u.shape, F32)
    for p in range(0, per, 2):
        both = jnp.dot(
            lhs, blk_ref[i, :, p * LANES : (p + 2) * LANES], preferred_element_type=F32
        )
        for k in range(2):
            part = both[:, k * LANES : (k + 1) * LANES]
            even += turned_down(part[:count], p + k, at)
            odd += turned_down(part[count:], p + k, at)
    odd = pltpu.roll(odd, HALF, axis=1)
    return even + jnp.where(low, turned_down(odd, 1, at), odd)


def ctx_index():
    at = 0
    for axis in CTX:
        at = at * lax.axis_size(axis) + lax.axis_index(axis)
    return at


def conv_kernel(size, sig_ref, taps_ref, skip_ref, blk_hbm, out_ref, sig, acc, blk, sems):
    count, rows = out_ref.shape[0], out_ref.shape[1]
    loads = [pltpu.make_async_copy(blk_hbm.at[c], blk.at[c], sems.at[c]) for c in range(rows)]
    for load in loads:
        load.start()
    me = ctx_index()
    sig[...] = sig_ref[...].reshape(count * 2 * rows, LANES).astype(F32)
    taps = taps_ref[...].astype(F32)
    group = lax.broadcasted_iota(jnp.int32, taps.shape, 0) == me * rows // size
    turned = rolled_rows(jnp.sum(jnp.where(group, taps, 0.0), axis=0, keepdims=True))
    own = upper()
    band = jnp.concatenate([jnp.where(own, 0.0, turned), jnp.where(own, turned, 0.0)], axis=0)
    band = band.astype(BF16)
    at = lax.broadcasted_iota(jnp.int32, (count, LANES), 0)
    lane = lax.broadcasted_iota(jnp.int32, skip_ref.shape, 1)
    for c in range(rows):
        product = sig[pl.ds(c, count, stride=2 * rows), :]
        gate = sig[pl.ds(rows + c, count, stride=2 * rows), :]
        both = jnp.concatenate([turned_down(product, 1, at), product], axis=1).astype(BF16)
        short = jnp.dot(both, band, preferred_element_type=F32)
        mid = (gate * short).astype(BF16).astype(F32)
        loads[c].wait()
        far = conv_channel(mid, blk, c).astype(BF16).astype(F32)
        skip = jnp.sum(
            jnp.where(lane == me * rows + c, skip_ref[...], 0.0), axis=1, keepdims=True
        )
        acc[pl.ds(c, count, stride=rows), :] = far + skip * mid
    out_ref[...] = acc[...].reshape(count, rows, LANES).astype(BF16)


def long_stage(signal, taps, skip, blocks, size):
    count, twice, _ = signal.shape
    rows = twice // 2
    vmem = pl.BlockSpec(memory_space=pltpu.VMEM)
    return pl.pallas_call(
        lambda *refs: conv_kernel(size, *refs),
        in_specs=[vmem, vmem, vmem, pl.BlockSpec(memory_space=pltpu.HBM)],
        out_specs=vmem,
        out_shape=jax.ShapeDtypeStruct((count, rows, LANES), BF16),
        scratch_shapes=[
            pltpu.VMEM((count * twice, LANES), F32),
            pltpu.VMEM((count * rows, LANES), F32),
            pltpu.VMEM(blocks.shape, BF16),
            pltpu.SemaphoreType.DMA((rows,)),
        ],
        name="long_stage",
        compiler_params=pltpu.CompilerParams(vmem_limit_bytes=24 << 20),
        cost_estimate=pl.CostEstimate(
            flops=8_000_000_000, bytes_accessed=blocks.size * 2, transcendentals=0
        ),
    )(signal, taps, skip, in_hbm(blocks))


def gate_kernel(near, long_ref, gate_ref, out_ref):
    channels = gate_ref.shape[1]
    tiles = []
    for b in range(channels // LANES):
        rows = slice(b * LANES, (b + 1) * LANES)
        whole = long_ref[rows, :].astype(F32).T
        gate = gate_ref[:, rows].astype(F32)
        tiles.append(gate * whole)
    half = LANES // 2
    low = lax.broadcasted_iota(jnp.int32, tiles[0].shape, 1) < half

    def piece(i, upper_half):
        tile = tiles[i // 2]
        return tile if (i % 2 == 1) == upper_half else pltpu.roll(tile, half, axis=1)

    for y in range(near):
        both = jnp.where(low, piece(y, False), piece(near + y, True)).astype(BF16)
        for copy in range(out_ref.shape[0]):
            out_ref[copy, :, y * LANES : (y + 1) * LANES] = both


def gate_stage(long_rows, gate, copies, near):
    tokens, channels = gate.shape
    return pl.pallas_call(
        lambda *refs: gate_kernel(near, *refs),
        out_shape=jax.ShapeDtypeStruct((copies, tokens, channels), BF16),
        name="gate_stage",
        compiler_params=pltpu.CompilerParams(vmem_limit_bytes=16 << 20),
        cost_estimate=pl.CostEstimate(
            flops=1_000_000_000, bytes_accessed=1 << 20, transcendentals=0
        ),
    )(long_rows, gate)


def project_own_kernel(feature_ref, weight_ref, part_ref, rest_ref, held, sems):
    core = lax.axis_index("core")
    blocks = feature_ref.shape[0]
    mine = [
        pltpu.make_async_copy(weight_ref.at[k, :, core], held.at[k], sems.at[0, k])
        for k in range(blocks)
    ]
    rest = [
        pltpu.make_async_copy(weight_ref.at[k, :, 1 - core], rest_ref.at[k], sems.at[1, k])
        for k in range(blocks)
    ]
    for copy in mine + rest:
        copy.start()
    total = jnp.zeros(part_ref.shape, F32)
    for k in range(blocks):
        mine[k].wait()
        weight = held[k].reshape(feature_ref.shape[2], part_ref.shape[1])
        total += jnp.dot(feature_ref[k], weight, preferred_element_type=F32)
    part_ref[...] = total
    for copy in rest:
        copy.wait()


def project_own(features, weight, near):
    blocks, tokens, channels = features.shape
    cols = weight.shape[1]
    parts = in_hbm(weight.reshape(blocks, near, 2, channels // near, cols))
    vmem = pl.BlockSpec(memory_space=pltpu.VMEM)
    half = (blocks, near, channels // near, cols)
    return pl.pallas_call(
        project_own_kernel,
        in_specs=[vmem, pl.BlockSpec(memory_space=pltpu.HBM)],
        out_specs=(vmem, vmem),
        out_shape=(
            jax.ShapeDtypeStruct((tokens, cols), F32),
            jax.ShapeDtypeStruct(half, weight.dtype),
        ),
        scratch_shapes=[
            pltpu.VMEM(half, weight.dtype),
            pltpu.SemaphoreType.DMA((2, blocks)),
        ],
        name="project_own",
        compiler_params=pltpu.CompilerParams(vmem_limit_bytes=8 << 20),
        cost_estimate=pl.CostEstimate(
            flops=4_000_000_000, bytes_accessed=weight.size * 2, transcendentals=0
        ),
    )(features, parts)


def project_other_kernel(feature_ref, weight_ref, part_ref, out_ref):
    total = part_ref[...]
    for k in range(feature_ref.shape[0]):
        weight = weight_ref[k].reshape(feature_ref.shape[2], out_ref.shape[1])
        total += jnp.dot(feature_ref[k], weight, preferred_element_type=F32)
    out_ref[...] = total.astype(BF16)


def project_other(features, weight, part):
    vmem = pl.BlockSpec(memory_space=pltpu.VMEM)
    return pl.pallas_call(
        project_other_kernel,
        in_specs=[vmem] * 3,
        out_specs=vmem,
        out_shape=jax.ShapeDtypeStruct(part.shape, BF16),
        name="project_other",
        compiler_params=pltpu.CompilerParams(vmem_limit_bytes=8 << 20),
    )(features, weight, part)


def in_hbm(value):
    return pltpu.with_memory_space_constraint(value, pltpu.HBM)


def to_each(parts, axes):
    return lax.all_to_all(parts, axes, 0, 0, tiled=True)


def shards(
    value_in, key_in, gate_short, gate_long, short_filter, long_filter, skip_gain, out_weight
):
    tokens, channels = value_in.shape
    ways = lax.axis_size(CTX)
    per_dev = channels // ways
    near = lax.axis_size("y")

    weight_rows = lax.all_gather(out_weight, "zh", axis=0, tiled=True)
    weight = lax.all_gather(weight_rows, ("x", "y"), axis=0, tiled=True)
    packed = pack(value_in, key_in, gate_short, per_dev)
    spread = to_each(packed, CTX)
    blocks = long_blocks(long_filter)
    long_part = long_stage(
        spread, short_filter, skip_gain[None, :], blocks, channels // short_filter.shape[0]
    )
    returned = to_each(long_part, CTX).reshape(channels, tokens)
    gated = gate_stage(returned, gate_long, lax.axis_size("zl"), near)
    own = to_each(gated, "zl")
    other = lax.ppermute(own, "core", [(0, 1), (1, 0)])
    part, rest = project_own(own, weight, near)
    return project_other(other, rest, part)


def solution(mesh):
    fine = Mesh(mesh.devices.reshape(4, 4, 4, 4, 2), CTX + CH)
    in_specs = (
        P(CTX, CH),
        P(CTX, CH),
        P(CTX, CH),
        P(CTX, CH),
        P(CH, None),
        P(CH + CTX, None),
        P(CH),
        P(CTX, CH),
    )
    return jax.shard_map(
        shards, mesh=fine, in_specs=in_specs, out_specs=P(CTX, CH), check_vma=False
    )
```
